256 devices in a mesh: tm: 16 (over z, core), space: 16 (over y, x).
Axes of the slice: x: 4, y: 4, z: 8, core: 2. Of those that a mesh axis runs over, the one named last changes fastest.
Arguments:
- initial: float32 [2, 512, 512], P(None, 'space'), may hold values from 0.2 to 1
- guess: float32 [256, 2, 512, 512], P('tm', None, 'space'), may hold values from 0 to 1
- kappa: float32 [2, 512, 512], P(None, 'space'), may hold values from 0.005 to 0.05
- feed: float32 [512, 512], P('space'), may hold values from 0.002 to 0.01
- kill: float32 [512, 512], P('space'), may hold values from 0.002 to 0.008
- react: float32 [512, 512], P('space'), may hold values from 0.002 to 0.008
Outputs:
- solution: float32 [256, 2, 512, 512], P('tm', None, 'space')
The draws below stay inside these ranges and needn't reach their ends.
All inputs are finite; a program needn't handle non-finite values.
Results may differ from the reference program's by a relative error of at most 0.00002.
Values sent between devices are 32-bit elements; how exact they have to be, the bound alone decides.
No kernel may reach another device: no remote copies, remote signals or barrier semaphores. Data moves between devices by JAX's collectives and lax.ppermute only.
A program may use at most 128 MiB of HBM per device.

```python
import math
import jax
import jax.numpy as jnp
from jax import lax

COLS = 512
SPAN = 8
NX = 512
NT = 256


def shard_levels(stream_key, extent, pieces, least, high):
    loudness = 1.0
    for dim, blocks in pieces:
        draws = jax.random.uniform(jax.random.fold_in(jax.random.fold_in(stream_key, 6), dim), (blocks,), jnp.float32, least / len(pieces), high / len(pieces))
        loudness = loudness * jnp.repeat(jnp.exp(draws), extent[dim] // blocks).reshape((-1,) + (1,) * (len(extent) - 1 - dim))
    return loudness


def setup_inputs(seed: int = 0) -> dict:
    streams_of = jax.random.split(jax.random.key(seed), 7)
    return {
        "initial": jnp.clip(0.2 + 0.8 * jax.random.uniform(streams_of[0], (2, NX, COLS), jnp.float32) ** shard_levels(streams_of[0], (2, NX, COLS), ((1, 16),), -0.2, 0.2), 0.2, 1.0),
        "guess": jnp.clip(1.0 * jax.random.uniform(streams_of[1], (NT, 2, NX, COLS), jnp.float32) ** shard_levels(streams_of[1], (NT, 2, NX, COLS), ((0, 16), (2, 16)), -0.2, 0.2), 0.0, 1.0),
        "kappa": jnp.clip(jnp.exp(math.log(0.05) - 2.3025851 * jax.random.uniform(streams_of[2], (2, NX, COLS), jnp.float32) ** shard_levels(streams_of[2], (2, NX, COLS), ((1, 16),), -0.2, 0.2)), 0.005, 0.05),
        "feed": jnp.clip(jnp.exp(math.log(0.01) - 1.6094378 * jax.random.uniform(streams_of[3], (NX, COLS), jnp.float32) ** shard_levels(streams_of[3], (NX, COLS), ((0, 16),), -0.2, 0.2)), 0.002, 0.01),
        "kill": jnp.clip(jnp.exp(math.log(0.008) - 1.3862944 * jax.random.uniform(streams_of[4], (NX, COLS), jnp.float32) ** shard_levels(streams_of[4], (NX, COLS), ((0, 16),), -0.2, 0.2)), 0.002, 0.008),
        "react": jnp.clip(jnp.exp(math.log(0.008) - 1.3862944 * jax.random.uniform(streams_of[5], (NX, COLS), jnp.float32) ** shard_levels(streams_of[5], (NX, COLS), ((0, 16),), -0.2, 0.2)), 0.002, 0.008),
    }


def coarsen(field):
    shape = field.shape
    blocks = field.reshape(shape[:-2] + (shape[-2] // 2, 2, shape[-1] // 2, 2))
    return blocks.mean(axis=(-3, -1))


def refine(field):
    return jnp.repeat(jnp.repeat(field, 2, axis=-2), 2, axis=-1)


def advance(state, row_padded, coeffs):
    spread, supply, removal, coupling = coeffs
    padded = jnp.pad(row_padded, [(0, 0)] * (row_padded.ndim - 1) + [(1, 1)])
    laplace = padded[..., :-2, 1:-1] + padded[..., 2:, 1:-1] + padded[..., 1:-1, :-2] + padded[..., 1:-1, 2:] - 4.0 * state
    first_species = state[..., 0, :, :]
    second_species = state[..., 1, :, :]
    coupled = coupling * first_species * second_species * second_species
    next_first = first_species + spread[0] * laplace[..., 0, :, :] - coupled + supply * (1.0 - first_species)
    next_second = second_species + spread[1] * laplace[..., 1, :, :] + coupled - (supply + removal) * second_species
    return jnp.stack([next_first, next_second], axis=-3)


def stepping(state, coeffs):
    row_padded = jnp.pad(state, [(0, 0)] * (state.ndim - 2) + [(1, 1), (0, 0)])
    return advance(state, row_padded, coeffs)


def relax_sweep(series, opening, coeffs, forcing):
    current = jnp.concatenate([opening[None], series[:-1, SPAN - 1]])
    columns = []
    for position in range(SPAN - 1):
        current = stepping(current, coeffs)
        if forcing is not None:
            current = current + forcing[:, position]
        columns.append(current)
    columns.append(series[:, SPAN - 1])
    return jnp.stack(columns, axis=1)


def reference(initial, guess, kappa, feed, kill, react):
    level_zero = (kappa, feed, kill, react)
    spread_one = coarsen(kappa)
    supply_one = coarsen(feed)
    removal_one = coarsen(kill)
    coupling_one = coarsen(react)
    level_one = (2.0 * spread_one, 8.0 * supply_one, 8.0 * removal_one, 8.0 * coupling_one)
    level_two = (4.0 * coarsen(spread_one), 64.0 * coarsen(supply_one), 64.0 * coarsen(removal_one), 64.0 * coarsen(coupling_one))
    count_one = guess.shape[0] // SPAN
    count_two = count_one // SPAN
    series = guess.reshape((count_one, SPAN) + guess.shape[1:])
    series = relax_sweep(series, initial, level_zero, None)
    series = series.at[:, SPAN - 1].set(stepping(series[:, SPAN - 2], level_zero))
    series = relax_sweep(series, initial, level_zero, None)
    ends = series[:, SPAN - 1]
    residual = stepping(series[:, SPAN - 2], level_zero) - ends
    restricted = coarsen(ends)
    start_one = coarsen(initial)
    earlier = jnp.concatenate([start_one[None], restricted[:-1]])
    forcing_one = coarsen(residual) + restricted - stepping(earlier, level_one)
    middle = restricted.reshape((count_two, SPAN) + restricted.shape[1:])
    forcing_grid = forcing_one.reshape(middle.shape)
    middle = relax_sweep(middle, start_one, level_one, forcing_grid)
    coarse_values = coarsen(middle[:, SPAN - 1])
    predicted = stepping(middle[:, SPAN - 2], level_one) + forcing_grid[:, SPAN - 1]
    coarse_right = coarsen(predicted - middle[:, SPAN - 1]) + coarse_values
    start_two = coarsen(start_one)
    coarse_prev = jnp.concatenate([start_two[None], coarse_values[:-1]])
    forcing_two = coarse_right - stepping(coarse_prev, level_two)

    def march(previous, forcing_step):
        following = stepping(previous, level_two) + forcing_step
        return following, following

    unused, solved = lax.scan(march, start_two, forcing_two)
    middle = middle.at[:, SPAN - 1].add(refine(solved - coarse_values))
    middle = relax_sweep(middle, start_one, level_one, forcing_grid)
    series = series.at[:, SPAN - 1].add(refine(middle.reshape(restricted.shape) - restricted))
    series = relax_sweep(series, initial, level_zero, None)
    return series.reshape(guess.shape)
```

```python
import jax
import jax.numpy as jnp
from jax import lax
from jax.experimental import pallas as pl
from jax.experimental.pallas import tpu as pltpu
from jax.sharding import Mesh
from jax.sharding import PartitionSpec as P

F32 = jnp.float32
AXES = ("k", "m", "space")
VMEM = pl.BlockSpec(memory_space=pltpu.VMEM)
SMEM = pl.BlockSpec(memory_space=pltpu.SMEM)
N_TM = 16
N_SPACE = 16
GROUP = 4
STRIP = 32


def exact_dot(x, matrix):
    high = x.astype(jnp.bfloat16)
    rest = x - high.astype(F32)
    middle = rest.astype(jnp.bfloat16)
    low = (rest - middle.astype(F32)).astype(jnp.bfloat16)

    def part(piece):
        return lax.dot_general(
            piece, matrix, (((1,), (0,)), ((), ())), preferred_element_type=F32
        )

    return part(low) + part(middle) + part(high)


def down_matrix(fine):
    rows = lax.broadcasted_iota(jnp.int32, (fine, fine // 2), 0)
    cols = lax.broadcasted_iota(jnp.int32, (fine, fine // 2), 1)
    inside = (rows == 2 * cols) | (rows == 2 * cols + 1)
    return jnp.where(inside, F32(0.25), F32(0.0)).astype(jnp.bfloat16)


def up_matrix(fine):
    rows = lax.broadcasted_iota(jnp.int32, (fine // 2, fine), 0)
    cols = lax.broadcasted_iota(jnp.int32, (fine // 2, fine), 1)
    inside = (cols == 2 * rows) | (cols == 2 * rows + 1)
    return jnp.where(inside, F32(1.0), F32(0.0)).astype(jnp.bfloat16)


def split_tiles(x):
    return [x[:, 128 * k : 128 * k + 128] for k in range(x.shape[1] // 128)]


def side_sums(tiles, lane_first, lane_last):
    right_going = [pltpu.roll(t, 1, 1) for t in tiles]
    left_going = [pltpu.roll(t, 127, 1) for t in tiles]
    zero = jnp.zeros_like(tiles[0])
    out = []
    for k in range(len(tiles)):
        before = right_going[k - 1] if k > 0 else zero
        after = left_going[k + 1] if k < len(tiles) - 1 else zero
        out.append(
            jnp.where(lane_first, before, right_going[k])
            + jnp.where(lane_last, after, left_going[k])
        )
    return out


def advance(load, store, coeffs, blocks, force=None):
    sub = lax.broadcasted_iota(jnp.int32, (8, 128), 0)
    lane = lax.broadcasted_iota(jnp.int32, (8, 128), 1)
    first_row, last_row = sub == 0, sub == 7
    first_lane, last_lane = lane == 0, lane == 127
    held = {}

    def fetch(i):
        if i not in held:
            species = []
            for x in load(i):
                tiles = split_tiles(x)
                species.append(
                    (
                        tiles,
                        [pltpu.roll(t, 1, 0) for t in tiles],
                        [pltpu.roll(t, 7, 0) for t in tiles],
                    )
                )
            held[i] = species
        return held[i]

    low, high = blocks
    for i in range(low, high):
        here = fetch(i)
        above = fetch(max(i - 1, low))
        below = fetch(min(i + 1, high - 1))
        held.pop(i - 2, None)
        c = coeffs(i)
        sums = []
        for q in range(2):
            tiles, down, up = here[q]
            sides = side_sums(tiles, first_lane, last_lane)
            sums.append(
                [
                    jnp.where(first_row, above[q][1][k], down[k])
                    + jnp.where(last_row, below[q][2][k], up[k])
                    + sides[k]
                    for k in range(len(tiles))
                ]
            )
        next_a, next_b = [], []
        spread_a, spread_b, supply, keep_a, keep_b, coupling = [split_tiles(x) for x in c]
        for k in range(len(sums[0])):
            a, b = here[0][0][k], here[1][0][k]
            coupled = coupling[k] * a * b * b
            next_a.append(keep_a[k] * a + spread_a[k] * sums[0][k] + (supply[k] - coupled))
            next_b.append(keep_b[k] * b + spread_b[k] * sums[1][k] + coupled)
        out = [jnp.concatenate(next_a, axis=1), jnp.concatenate(next_b, axis=1)]
        if force is not None:
            extra = force(i)
            out = [out[0] + extra[0], out[1] + extra[1]]
        store(i, out)


def derived(spread_a, spread_b, supply, removal, coupling):
    return (
        spread_a,
        spread_b,
        supply,
        1.0 - supply - 4.0 * spread_a,
        1.0 - supply - removal - 4.0 * spread_b,
        coupling,
    )


def block(i):
    return slice(8 * i, 8 * i + 8)


class Rows:
    def __init__(self, ref):
        self.ref, self.used = ref, 0

    def coarsen(self, x):
        count = x.shape[0]
        parts = []
        for tile in split_tiles(x):
            n = self.used
            self.used += 1
            self.ref[n, 0:count] = tile
            even = self.ref[n, pl.ds(0, count // 2, stride=2)]
            parts.append(even + self.ref[n, pl.ds(1, count // 2, stride=2)])
        return jnp.concatenate(parts, axis=1)

    def repeat(self, x):
        count = x.shape[0]
        parts = []
        for tile in split_tiles(x):
            n = self.used
            self.used += 1
            self.ref[n, pl.ds(0, count, stride=2)] = tile
            self.ref[n, pl.ds(1, count, stride=2)] = tile
            parts.append(self.ref[n, 0 : 2 * count])
        return jnp.concatenate(parts, axis=1)


def fine_kernel(
    where_ref, shift_ref, dlo_ref, dhi_ref, nlo_ref, nhi_ref, own_ref, coef_ref,
    a01_ref, a2_ref, w01_ref, w2_ref, send_ref, fine_ref,
    s0, s1, raw, tall, mid_state, mid_coef, cells,
):
    rows = Rows(cells)
    opening = where_ref[0] == 0
    for c in range(2):
        for q in range(2):
            s0[c, q, 0:16] = dlo_ref[2 * c + q]
            s0[c, q, 16:48] = shift_ref[2 * c + q]
            s0[c, q, 48:64] = dhi_ref[2 * c + q]
    for q in range(2):
        s0[2, q, 0:16] = nlo_ref[5 + q]
        s0[2, q, 16:48] = own_ref[q]
        s0[2, q, 48:64] = nhi_ref[5 + q]
    for f in range(5):
        raw[f, 0:16] = nlo_ref[f]
        raw[f, 16:48] = coef_ref[f]
        raw[f, 48:64] = nhi_ref[f]
    for i in range(8):
        r = block(i)
        parts = derived(*[raw[f, r] for f in range(5)])
        for n in range(6):
            tall[n, r] = parts[n]
        if 1 <= i < 7:
            for n in range(6):
                fine_ref[n, block(i - 1)] = parts[n]

    def coeffs(i):
        return [tall[n, block(i)] for n in range(6)]

    def run(source, target, chain, blocks):
        def load(i):
            return [source[chain, q, block(i)] for q in range(2)]

        def store(i, values):
            for q in range(2):
                target[chain, q, block(i)] = values[q]

        advance(load, store, coeffs, blocks)

    def first_pair(n, carry):
        for source, target in ((s0, s1), (s1, s0)):
            run(source, target, 0, (0, 8))
            run(source, target, 1, (0, 8))
            run(source, target, 2, (1, 7))
        return carry

    lax.fori_loop(0, 4, first_pair, 0)

    for q in range(2):
        s0[0, q, 0:16] = jnp.where(opening, dlo_ref[q], s0[0, q, 0:16])
        s0[0, q, 16:48] = jnp.where(opening, shift_ref[q], s0[0, q, 16:48])
        s0[0, q, 48:64] = jnp.where(opening, dhi_ref[q], s0[0, q, 48:64])
    for q in range(2):
        for c in range(2):
            a01_ref[c, q] = s0[c, q, 8:56]
        a2_ref[q] = s0[2, q, 16:48]

    down = down_matrix(512)
    stacked = jnp.concatenate([rows.coarsen(raw[f]) for f in range(5)], axis=0)
    coarse = exact_dot(stacked, down)
    for f in range(5):
        send_ref[6 + f] = coarse[32 * f + 8 : 32 * f + 24]
    for i in range(4):
        at = [coarse[32 * f + 8 * i : 32 * f + 8 * i + 8] for f in range(5)]
        parts = derived(2.0 * at[0], 2.0 * at[1], 8.0 * at[2], 8.0 * at[3], 8.0 * at[4])
        for n in range(6):
            mid_coef[n, block(i)] = parts[n]
    stacked = jnp.concatenate(
        [rows.coarsen(s0[c, q]) for c in range(2) for q in range(2)]
        + [rows.coarsen(s0[2, q, 16:48]) for q in range(2)],
        axis=0,
    )
    coarse = exact_dot(stacked, down)
    for c in range(2):
        for q in range(2):
            mid_state[c, q] = coarse[32 * (2 * c + q) : 32 * (2 * c + q) + 32]
    for q in range(2):
        w2_ref[q] = coarse[128 + 16 * q : 144 + 16 * q]
    for c in range(2):
        for q in range(2):
            w01_ref[c, q] = mid_state[c, q, 4:28]
    for q in range(2):
        send_ref[4 + q] = mid_state[0, q, 8:24]

    def second_pair(n, carry):
        for source, target in ((s0, s1), (s1, s0)):
            run(source, target, 0, (1, 7))
            run(source, target, 1, (1, 7))
        return carry

    lax.fori_loop(0, 4, second_pair, 0)

    for q in range(2):
        s0[0, q, 16:48] = s0[0, q, 16:48] - a01_ref[1, q, 8:40]
        s0[1, q, 16:48] = s0[1, q, 16:48] - a2_ref[q]
    stacked = jnp.concatenate(
        [rows.coarsen(s0[c, q, 16:48]) for c in range(2) for q in range(2)], axis=0
    )
    coarse = exact_dot(stacked, down)
    for c in range(2):
        for q in range(2):
            at = coarse[16 * (2 * c + q) : 16 * (2 * c + q) + 16]
            end = mid_state[1, q, 8:24] if c == 0 else w2_ref[q]
            send_ref[2 * c + q] = at + end

    for c in range(2):

        def load(i):
            return [mid_state[c, q, block(i)] for q in range(2)]

        def store(i, values):
            if 1 <= i < 3:
                for q in range(2):
                    send_ref[2 * c + q, block(i - 1)] = (
                        send_ref[2 * c + q, block(i - 1)] - values[q]
                    )

        advance(load, store, lambda i: [mid_coef[n, block(i)] for n in range(6)], (0, 4))


def wide_mid_coefs(raw, coef_ref, lo_ref, hi_ref, mid_coef):
    for f in range(5):
        raw[f, 0:16] = lo_ref[6 + f]
        raw[f, 16:32] = coef_ref[6 + f]
        raw[f, 32:48] = hi_ref[6 + f]
    at = [raw[f, 4:44] for f in range(5)]
    parts = derived(2.0 * at[0], 2.0 * at[1], 8.0 * at[2], 8.0 * at[3], 8.0 * at[4])
    for n in range(6):
        mid_coef[n] = parts[n]


def mid_kernel(
    gathered_ref, own_ref, lo_ref, hi_ref, out_ref, coef_out_ref, raw, state, cells,
):
    rows = Rows(cells)
    wide_mid_coefs(raw, own_ref, lo_ref, hi_ref, coef_out_ref)

    def coeffs(i):
        return [coef_out_ref[n, block(i)] for n in range(6)]

    for step in range(8):
        holder, place = step // 2, step % 2

        def load(i):
            if step == 0:
                return [gathered_ref[0, 4 + q, block(i)] for q in range(2)]
            return [state[(step + 1) % 2, q, block(i)] for q in range(2)]

        def force(i):
            return [gathered_ref[holder, 2 * place + q, block(i)] for q in range(2)]

        def store(i, values):
            for q in range(2):
                state[step % 2, q, block(i)] = values[q]

        advance(load, store, coeffs, (0, 5), force)
    stacked = jnp.concatenate(
        [rows.coarsen(state[1, q, 12:28]) for q in range(2)]
        + [rows.coarsen(gathered_ref[0, 4 + q, 12:28]) for q in range(2)],
        axis=0,
    )
    coarse = exact_dot(stacked, down_matrix(256))
    for f in range(4):
        out_ref[f] = coarse[8 * f : 8 * f + 8]


def final_kernel(
    where_ref, gathered_ref, top_ref, pred_ref, mid_coef, own_ref, lo_ref, hi_ref,
    a01_ref, a2_ref, w01_ref, w2_ref, fine_ref,
    out_ref,
    raw, low_coef, yz, series, cells, fine,
):
    rows = Rows(cells)
    k, m = where_ref[1], where_ref[2]
    for f in range(5):
        raw[f, 0:16] = lo_ref[6 + f]
        raw[f, 16:32] = own_ref[6 + f]
        raw[f, 32:48] = hi_ref[6 + f]
    down = down_matrix(256)
    up_low = up_matrix(256)
    stacked = jnp.concatenate([rows.coarsen(raw[f]) for f in range(5)], axis=0)
    coarse = exact_dot(stacked, down)
    at = [coarse[24 * f : 24 * f + 24] for f in range(5)]
    parts = derived(4.0 * at[0], 4.0 * at[1], 64.0 * at[2], 64.0 * at[3], 64.0 * at[4])
    for n in range(6):
        low_coef[n] = parts[n]

    def low_step(slot, target):
        def load(i):
            return [yz[slot, q, block(i)] for q in range(2)]

        def store(i, values):
            for q in range(2):
                yz[target, q, block(i)] = values[q]

        advance(load, store, lambda i: [low_coef[n, block(i)] for n in range(6)], (0, 3))

    for q in range(2):
        yz[0, q] = jnp.zeros((24, 128), F32)
    for back in (2, 1, 0):
        behind = k - 1 - back
        follows = jnp.where(behind > 0, F32(1.0), F32(0.0))
        for q in range(2):
            for piece in range(3):
                yz[1, q, block(piece)] = top_ref[back, piece, 2 + q]
        low_step(0, 2)
        low_step(1, 3)
        for q in range(2):
            for piece in range(3):
                r = block(piece)
                yz[0, q, r] = top_ref[back, piece, q] + follows * (yz[2, q, r] - yz[3, q, r])
    stacked = jnp.concatenate(
        [rows.coarsen(gathered_ref[0, 4 + q]) for q in range(2)]
        + [rows.coarsen(w2_ref[q]) for q in range(2)]
        + [jnp.zeros((8, 256), F32)],
        axis=0,
    )
    coarse = exact_dot(stacked, down)
    inner = jnp.where(k > 0, F32(1.0), F32(0.0))
    fixes = []
    for q in range(2):
        z = coarse[20 * q : 20 * q + 20]
        yz[1, q] = jnp.zeros((24, 128), F32)
        yz[1, q, 2:22] = z
        fixes.append(inner * (yz[0, q, 2:22] - z))
    low_step(0, 2)
    low_step(1, 3)
    for q in range(2):
        r = block(1)
        end = pred_ref[q] + inner * (yz[2, q, r] - yz[3, q, r])
        fixes.append(end - coarse[40 + 8 * q : 48 + 8 * q])
    fixes.append(jnp.zeros((8, 128), F32))
    refined = exact_dot(jnp.concatenate(fixes, axis=0), up_low)
    for q in range(2):
        series[0, q] = gathered_ref[0, 4 + q] + rows.repeat(refined[20 * q : 20 * q + 20])
        end = rows.repeat(refined[40 + 8 * q : 48 + 8 * q])
        series[8, q, 12:28] = w2_ref[q] + end

    for step in range(7):
        holder, place = step // 2, step % 2

        def load(i):
            return [series[step, q, block(i)] for q in range(2)]

        def force(i):
            return [gathered_ref[holder, 2 * place + q, block(i)] for q in range(2)]

        def store(i, values):
            for q in range(2):
                series[step + 1, q, block(i)] = values[q]

        advance(
            load, store, lambda i: [mid_coef[n, block(i)] for n in range(6)], (0, 5), force
        )

    changes = []
    for c in range(2):
        for q in range(2):
            changes.append(series[2 * m + c, q, 8:32] - w01_ref[c, q])
    for q in range(2):
        changes.append(series[2 * m + 2, q, 12:28] - w2_ref[q])
    refined = exact_dot(jnp.concatenate(changes, axis=0), up_matrix(512))
    for c in range(2):
        for q in range(2):
            n = 2 * c + q
            fine[0, c, q] = a01_ref[c, q] + rows.repeat(refined[24 * n : 24 * n + 24])
    for q in range(2):
        out_ref[15, q] = a2_ref[q] + rows.repeat(refined[96 + 16 * q : 112 + 16 * q])
        out_ref[7, q] = fine[0, 1, q, 8:40]

    def fine_step(source, target, position):
        for c in range(2):

            def load(i):
                return [fine[source, c, q, block(i)] for q in range(2)]

            def store(i, values):
                for q in range(2):
                    fine[target, c, q, block(i)] = values[q]
                    if 1 <= i < 5:
                        out_ref[8 * c + position, q, block(i - 1)] = values[q]

            advance(load, store, lambda i: [fine_ref[n, block(i)] for n in range(6)], (0, 6))

    def pair(n, carry):
        fine_step(0, 1, 2 * n)
        fine_step(1, 0, 2 * n + 1)
        return carry

    lax.fori_loop(0, 3, pair, 0)
    fine_step(0, 1, 6)


def struct(*shape):
    return jax.ShapeDtypeStruct(shape, F32)


def scratch(*shape):
    return pltpu.VMEM(shape, F32)


def device(t, s):
    return t * N_SPACE + s


def send(x, dt, ds):
    pairs = [
        (device(t, s), device((t + dt) % N_TM, s + ds))
        for t in range(N_TM)
        for s in range(N_SPACE)
        if 0 <= s + ds < N_SPACE
    ]
    return lax.ppermute(x, AXES, pairs)


def from_group_behind(x, ds):
    pairs = []
    for k in range(GROUP):
        for m in range(k):
            for s in range(N_SPACE):
                if 0 <= s + ds < N_SPACE:
                    pairs.append((device(4 * (k - 1 - m) + m, s + ds), device(4 * k + m, s)))
    return lax.ppermute(x, AXES, pairs)


def local(initial, guess, kappa, feed, kill, react):
    k, m = lax.axis_index("k"), lax.axis_index("m")
    t = GROUP * k + m
    where = jnp.stack([t, k, m]).astype(jnp.int32)
    coef = jnp.concatenate([kappa, feed[None], kill[None], react[None]])
    first_end = guess[7]
    ends = jnp.concatenate([first_end, guess[15]])
    sent = jnp.where(t == N_TM - 1, jnp.concatenate([initial, initial]), ends)
    beside = jnp.concatenate([coef, first_end])
    nlo = send(beside[:, 16:], 0, 1)
    nhi = send(beside[:, :16], 0, -1)
    dlo = send(sent[:, 16:], 1, 1)
    dhi = send(sent[:, :16], 1, -1)
    shift = send(sent, 1, 0)
    a01, a2, w01, w2, packed, fine = pl.pallas_call(
        fine_kernel,
        out_shape=(
            struct(2, 2, 48, 512), struct(2, 32, 512), struct(2, 2, 24, 256),
            struct(2, 16, 256), struct(11, 16, 256), struct(6, 48, 512),
        ),
        in_specs=[SMEM] + [VMEM] * 7,
        out_specs=(VMEM,) * 6,
        scratch_shapes=[
            scratch(3, 2, 64, 512), scratch(3, 2, 64, 512), scratch(5, 64, 512),
            scratch(6, 64, 512), scratch(2, 2, 32, 256), scratch(6, 32, 256), scratch(60, 64, 128),
        ],
    )(where, shift, dlo, dhi, nlo, nhi, first_end, coef)
    lo = send(packed, 0, 1)
    hi = send(packed, 0, -1)
    window = jnp.concatenate([lo[:6, 4:], packed[:6], hi[:6, :12]], axis=1)
    gathered = lax.all_gather(window, "m", axis=0, tiled=False)
    pred, mid_coef = pl.pallas_call(
        mid_kernel,
        out_shape=(struct(4, 8, 128), struct(6, 40, 256)),
        in_specs=[VMEM] * 4,
        out_specs=(VMEM,) * 2,
        scratch_shapes=[scratch(5, 48, 256), scratch(2, 2, 40, 256), scratch(8, 16, 128)],
    )(gathered, packed, lo, hi)
    pieces = [from_group_behind(pred, ds) for ds in (-1, 0, 1)]
    top = lax.all_gather(jnp.stack(pieces), "m", axis=0, tiled=False)
    return pl.pallas_call(
        final_kernel,
        out_shape=struct(16, 2, 32, 512),
        in_specs=[SMEM] + [VMEM] * 12,
        out_specs=VMEM,
        scratch_shapes=[
            scratch(5, 48, 256), scratch(6, 24, 128), scratch(4, 2, 24, 128),
            scratch(9, 2, 40, 256), scratch(50, 48, 128), scratch(2, 2, 2, 48, 512),
        ],
    )(where, gathered, top, pred, mid_coef, packed, lo, hi, a01, a2, w01, w2, fine)


def solution(mesh):
    split = Mesh(mesh.devices.reshape(4, 4, 16), AXES)
    tm = ("k", "m")
    placed = (
        P(None, "space", None),
        P(tm, None, "space", None),
        P(None, "space", None),
        P("space", None),
        P("space", None),
        P("space", None),
    )
    return jax.shard_map(
        local, mesh=split, in_specs=placed, out_specs=P(tm, None, "space", None), check_vma=False
    )
```

```python
import jax
import jax.numpy as jnp
from jax import lax
from jax.experimental import pallas as pl
from jax.experimental.pallas import tpu as pltpu
from jax.sharding import Mesh
from jax.sharding import PartitionSpec as P

F32 = jnp.float32
AXES = ("k", "m", "space")
VMEM = pl.BlockSpec(memory_space=pltpu.VMEM)
ANY = pl.BlockSpec(memory_space=pl.ANY)
SMEM = pl.BlockSpec(memory_space=pltpu.SMEM)
N_TM = 16
N_SPACE = 16
GROUP = 4
STRIP = 32


def exact_dot(x, matrix):
    high = x.astype(jnp.bfloat16)
    rest = x - high.astype(F32)
    middle = rest.astype(jnp.bfloat16)
    low = (rest - middle.astype(F32)).astype(jnp.bfloat16)

    def part(piece):
        return lax.dot_general(
            piece, matrix, (((1,), (0,)), ((), ())), preferred_element_type=F32
        )

    return part(low) + part(middle) + part(high)


def down_matrix(fine):
    rows = lax.broadcasted_iota(jnp.int32, (fine, fine // 2), 0)
    cols = lax.broadcasted_iota(jnp.int32, (fine, fine // 2), 1)
    inside = (rows == 2 * cols) | (rows == 2 * cols + 1)
    return jnp.where(inside, F32(0.25), F32(0.0)).astype(jnp.bfloat16)


def up_matrix(fine):
    rows = lax.broadcasted_iota(jnp.int32, (fine // 2, fine), 0)
    cols = lax.broadcasted_iota(jnp.int32, (fine // 2, fine), 1)
    inside = (cols == 2 * rows) | (cols == 2 * rows + 1)
    return jnp.where(inside, F32(1.0), F32(0.0)).astype(jnp.bfloat16)


def split_tiles(x):
    return [x[:, 128 * k : 128 * k + 128] for k in range(x.shape[1] // 128)]


def side_sums(tiles, lane_first, lane_last):
    right_going = [pltpu.roll(t, 1, 1) for t in tiles]
    left_going = [pltpu.roll(t, 127, 1) for t in tiles]
    zero = jnp.zeros_like(tiles[0])
    out = []
    for k in range(len(tiles)):
        before = right_going[k - 1] if k > 0 else zero
        after = left_going[k + 1] if k < len(tiles) - 1 else zero
        out.append(
            jnp.where(lane_first, before, right_going[k])
            + jnp.where(lane_last, after, left_going[k])
        )
    return out


def advance(load, store, coeffs, blocks, force=None):
    sub = lax.broadcasted_iota(jnp.int32, (8, 128), 0)
    lane = lax.broadcasted_iota(jnp.int32, (8, 128), 1)
    first_row, last_row = sub == 0, sub == 7
    first_lane, last_lane = lane == 0, lane == 127
    held = {}

    def fetch(i):
        if i not in held:
            species = []
            for x in load(i):
                tiles = split_tiles(x)
                species.append(
                    (
                        tiles,
                        [pltpu.roll(t, 1, 0) for t in tiles],
                        [pltpu.roll(t, 7, 0) for t in tiles],
                    )
                )
            held[i] = species
        return held[i]

    low, high = blocks
    for i in range(low, high):
        here = fetch(i)
        above = fetch(max(i - 1, low))
        below = fetch(min(i + 1, high - 1))
        held.pop(i - 2, None)
        c = coeffs(i)
        sums = []
        for q in range(2):
            tiles, down, up = here[q]
            sides = side_sums(tiles, first_lane, last_lane)
            sums.append(
                [
                    jnp.where(first_row, above[q][1][k], down[k])
                    + jnp.where(last_row, below[q][2][k], up[k])
                    + sides[k]
                    for k in range(len(tiles))
                ]
            )
        next_a, next_b = [], []
        spread_a, spread_b, supply, keep_a, keep_b, coupling = [split_tiles(x) for x in c]
        for k in range(len(sums[0])):
            a, b = here[0][0][k], here[1][0][k]
            coupled = coupling[k] * a * b * b
            next_a.append(keep_a[k] * a + spread_a[k] * sums[0][k] + (supply[k] - coupled))
            next_b.append(keep_b[k] * b + spread_b[k] * sums[1][k] + coupled)
        out = [jnp.concatenate(next_a, axis=1), jnp.concatenate(next_b, axis=1)]
        if force is not None:
            extra = force(i)
            out = [out[0] + extra[0], out[1] + extra[1]]
        store(i, out)


def derived(spread_a, spread_b, supply, removal, coupling):
    return (
        spread_a,
        spread_b,
        supply,
        1.0 - supply - 4.0 * spread_a,
        1.0 - supply - removal - 4.0 * spread_b,
        coupling,
    )


def block(i):
    return slice(8 * i, 8 * i + 8)


class Rows:
    def __init__(self, ref):
        self.ref, self.used = ref, 0

    def coarsen(self, x):
        count = x.shape[0]
        parts = []
        for tile in split_tiles(x):
            n = self.used
            self.used += 1
            self.ref[n, 0:count] = tile
            even = self.ref[n, pl.ds(0, count // 2, stride=2)]
            parts.append(even + self.ref[n, pl.ds(1, count // 2, stride=2)])
        return jnp.concatenate(parts, axis=1)

    def repeat(self, x):
        count = x.shape[0]
        parts = []
        for tile in split_tiles(x):
            n = self.used
            self.used += 1
            self.ref[n, pl.ds(0, count, stride=2)] = tile
            self.ref[n, pl.ds(1, count, stride=2)] = tile
            parts.append(self.ref[n, 0 : 2 * count])
        return jnp.concatenate(parts, axis=1)


def pack_kernel(
    where_ref, initial_ref, guess_ref, kappa_ref, feed_ref, kill_ref, react_ref,
    own_ref, low_ref, high_ref, sems,
):
    last = where_ref[0] == N_TM - 1
    count = [0]

    def copy(source, target):
        n = count[0]
        count[0] += 1
        return pltpu.make_async_copy(source, target, sems.at[n])

    def copies(pick, place, many):
        out = []
        at = pl.ds(place, many) if many > 1 else place
        for target, low, size in ((own_ref, 0, 32), (low_ref, 16, 16), (high_ref, 0, 16)):
            out.append(copy(pick(pl.ds(low, size)), target.at[at]))
        return out

    plain = []
    plain += copies(lambda r: guess_ref.at[7, :, r], 5, 2)
    plain += copies(lambda r: kappa_ref.at[:, r], 0, 2)
    plain += copies(lambda r: feed_ref.at[r], 2, 1)
    plain += copies(lambda r: kill_ref.at[r], 3, 1)
    plain += copies(lambda r: react_ref.at[r], 4, 1)
    for c in plain:
        c.start()
    mark = count[0]
    ends = copies(lambda r: guess_ref.at[15, :, r], 7, 2)
    count[0] = mark
    starts = copies(lambda r: initial_ref.at[:, r], 7, 2)

    @pl.when(last)
    def _():
        for c in starts:
            c.start()

    @pl.when(jnp.logical_not(last))
    def _():
        for c in ends:
            c.start()

    for c in plain + ends:
        c.wait()


def fine_kernel(
    where_ref, own_ref, lo_ref, hi_ref,
    a01_ref, a2_ref, w2_ref, packed_ref, send_ref, fine_ref,
    s0, s1, raw, tall, mid_state, mid_coef, cells,
):
    rows = Rows(cells)
    last = where_ref[0] == N_TM - 1
    for c in range(2):
        for q in range(2):
            f = 5 + 2 * c + q
            s0[c, q, 0:16] = lo_ref[f]
            s0[c, q, 16:48] = own_ref[f]
            s0[c, q, 48:64] = hi_ref[f]
    for f in range(5):
        raw[f, 0:16] = lo_ref[f]
        raw[f, 16:48] = own_ref[f]
        raw[f, 48:64] = hi_ref[f]
    for i in range(8):
        r = block(i)
        parts = derived(*[raw[f, r] for f in range(5)])
        for n in range(6):
            tall[n, r] = parts[n]
        if 1 <= i < 7:
            for n in range(6):
                fine_ref[n, block(i - 1)] = parts[n]

    def coeffs(i):
        return [tall[n, block(i)] for n in range(6)]

    def run(source, target, chain, blocks):
        def load(i):
            return [source[chain, q, block(i)] for q in range(2)]

        def store(i, values):
            for q in range(2):
                target[chain, q, block(i)] = values[q]

        advance(load, store, coeffs, blocks)

    def first_pair(n, carry):
        for source, target in ((s0, s1), (s1, s0)):
            run(source, target, 0, (0, 8))
            run(source, target, 1, (0, 8))
        return carry

    lax.fori_loop(0, 4, first_pair, 0)

    for q in range(2):
        a2_ref[q] = s0[0, q, 16:48]
    stacked = [rows.coarsen(s0[0, q, 16:48]) for q in range(2)]
    for q in range(2):
        s0[0, q, 0:16] = jnp.where(last, lo_ref[7 + q], s0[0, q, 0:16])
        s0[0, q, 16:48] = jnp.where(last, own_ref[7 + q], s0[0, q, 16:48])
        s0[0, q, 48:64] = jnp.where(last, hi_ref[7 + q], s0[0, q, 48:64])
    for q in range(2):
        for c in range(2):
            a01_ref[c, q, 0:48] = s0[c, q, 8:56]

    stacked += [rows.coarsen(raw[f]) for f in range(5)]
    stacked += [rows.coarsen(s0[c, q]) for c in range(2) for q in range(2)]
    down = down_matrix(512)
    coarse = exact_dot(jnp.concatenate(stacked, axis=0), down)
    for q in range(2):
        w2_ref[q] = coarse[16 * q : 16 * q + 16]
    base = 32
    for f in range(5):
        send_ref[6 + f] = coarse[base + 32 * f + 8 : base + 32 * f + 24]
    for i in range(4):
        at = [coarse[base + 32 * f + 8 * i : base + 32 * f + 8 * i + 8] for f in range(5)]
        parts = derived(2.0 * at[0], 2.0 * at[1], 8.0 * at[2], 8.0 * at[3], 8.0 * at[4])
        for n in range(6):
            mid_coef[n, block(i)] = parts[n]
    base = 192
    for c in range(2):
        for q in range(2):
            n = base + 32 * (2 * c + q)
            mid_state[c, q] = coarse[n : n + 32]
            a01_ref[c, q, 48:60, 0:256] = coarse[n + 4 : n + 16]
            a01_ref[c, q, 48:60, 256:512] = coarse[n + 16 : n + 28]
    for q in range(2):
        send_ref[4 + q] = mid_state[0, q, 8:24]
        packed_ref[4 + q] = mid_state[0, q, 8:24]

    def second_pair(n, carry):
        for source, target in ((s0, s1), (s1, s0)):
            run(source, target, 0, (1, 7))
            run(source, target, 1, (1, 7))
        return carry

    lax.fori_loop(0, 4, second_pair, 0)

    stacked = jnp.concatenate(
        [rows.coarsen(s0[c, q, 16:48]) for c in range(2) for q in range(2)], axis=0
    )
    coarse = exact_dot(stacked, down)
    for c in range(2):

        def load(i):
            return [mid_state[c, q, block(i)] for q in range(2)]

        def store(i, values):
            if 1 <= i < 3:
                for q in range(2):
                    n = 16 * (2 * c + q) + 8 * (i - 1)
                    forcing = coarse[n : n + 8] - values[q]
                    send_ref[2 * c + q, block(i - 1)] = forcing
                    packed_ref[2 * c + q, block(i - 1)] = forcing

        advance(load, store, lambda i: [mid_coef[n, block(i)] for n in range(6)], (0, 4))


def wide_mid_coefs(raw, coef_ref, lo_ref, hi_ref, mid_coef):
    for f in range(5):
        raw[f, 0:16] = lo_ref[6 + f]
        raw[f, 16:32] = coef_ref[6 + f]
        raw[f, 32:48] = hi_ref[6 + f]
    at = [raw[f, 4:44] for f in range(5)]
    parts = derived(2.0 * at[0], 2.0 * at[1], 8.0 * at[2], 8.0 * at[3], 8.0 * at[4])
    for n in range(6):
        mid_coef[n] = parts[n]


def mid_kernel(
    gathered_ref, own_ref, lo_ref, hi_ref, out_ref, coef_out_ref, raw, state, cells,
):
    rows = Rows(cells)
    wide_mid_coefs(raw, own_ref, lo_ref, hi_ref, coef_out_ref)

    def coeffs(i):
        return [coef_out_ref[n, block(i)] for n in range(6)]

    for step in range(8):
        holder, place = step // 2, step % 2

        def load(i):
            if step == 0:
                return [gathered_ref[0, 4 + q, block(i)] for q in range(2)]
            return [state[(step + 1) % 2, q, block(i)] for q in range(2)]

        def force(i):
            return [gathered_ref[holder, 2 * place + q, block(i)] for q in range(2)]

        def store(i, values):
            for q in range(2):
                state[step % 2, q, block(i)] = values[q]

        advance(load, store, coeffs, (0, 5), force)
    stacked = jnp.concatenate(
        [rows.coarsen(state[1, q, 12:28]) for q in range(2)]
        + [rows.coarsen(gathered_ref[0, 4 + q, 12:28]) for q in range(2)],
        axis=0,
    )
    coarse = exact_dot(stacked, down_matrix(256))
    for f in range(4):
        out_ref[f] = coarse[8 * f : 8 * f + 8]


def final_kernel(
    where_ref, gathered_ref, top_ref, pred_ref, mid_coef, own_ref, lo_ref, hi_ref,
    a01_ref, a2_ref, w2_ref, fine_ref,
    result_ref,
    raw, low_coef, yz, series, cells, fine, w01, out_ref, sems,
):
    rows = Rows(cells)
    k, m = where_ref[1], where_ref[2]
    for f in range(5):
        raw[f, 0:16] = lo_ref[6 + f]
        raw[f, 16:32] = own_ref[6 + f]
        raw[f, 32:48] = hi_ref[6 + f]
    down = down_matrix(256)
    up_low = up_matrix(256)
    stacked = jnp.concatenate([rows.coarsen(raw[f]) for f in range(5)], axis=0)
    coarse = exact_dot(stacked, down)
    at = [coarse[24 * f : 24 * f + 24] for f in range(5)]
    parts = derived(4.0 * at[0], 4.0 * at[1], 64.0 * at[2], 64.0 * at[3], 64.0 * at[4])
    for n in range(6):
        low_coef[n] = parts[n]

    def low_step(slot, target):
        def load(i):
            return [yz[slot, q, block(i)] for q in range(2)]

        def store(i, values):
            for q in range(2):
                yz[target, q, block(i)] = values[q]

        advance(load, store, lambda i: [low_coef[n, block(i)] for n in range(6)], (0, 3))

    for q in range(2):
        yz[0, q] = jnp.zeros((24, 128), F32)
    for back in (2, 1, 0):
        behind = k - 1 - back
        follows = jnp.where(behind > 0, F32(1.0), F32(0.0))
        for q in range(2):
            for piece in range(3):
                yz[1, q, block(piece)] = top_ref[back, piece, 2 + q]
        low_step(0, 2)
        low_step(1, 3)
        for q in range(2):
            for piece in range(3):
                r = block(piece)
                yz[0, q, r] = top_ref[back, piece, q] + follows * (yz[2, q, r] - yz[3, q, r])
    stacked = jnp.concatenate(
        [rows.coarsen(gathered_ref[0, 4 + q]) for q in range(2)]
        + [rows.coarsen(w2_ref[q]) for q in range(2)]
        + [jnp.zeros((8, 256), F32)],
        axis=0,
    )
    coarse = exact_dot(stacked, down)
    inner = jnp.where(k > 0, F32(1.0), F32(0.0))
    fixes = []
    for q in range(2):
        z = coarse[20 * q : 20 * q + 20]
        yz[1, q] = jnp.zeros((24, 128), F32)
        yz[1, q, 2:22] = z
        fixes.append(inner * (yz[0, q, 2:22] - z))
    low_step(0, 2)
    low_step(1, 3)
    for q in range(2):
        r = block(1)
        end = pred_ref[q] + inner * (yz[2, q, r] - yz[3, q, r])
        fixes.append(end - coarse[40 + 8 * q : 48 + 8 * q])
    fixes.append(jnp.zeros((8, 128), F32))
    refined = exact_dot(jnp.concatenate(fixes, axis=0), up_low)
    for q in range(2):
        series[0, q] = gathered_ref[0, 4 + q] + rows.repeat(refined[20 * q : 20 * q + 20])
        end = rows.repeat(refined[40 + 8 * q : 48 + 8 * q])
        series[8, q, 12:28] = w2_ref[q] + end

    for step in range(7):
        holder, place = step // 2, step % 2

        def load(i):
            return [series[step, q, block(i)] for q in range(2)]

        def force(i):
            return [gathered_ref[holder, 2 * place + q, block(i)] for q in range(2)]

        def store(i, values):
            for q in range(2):
                series[step + 1, q, block(i)] = values[q]

        advance(
            load, store, lambda i: [mid_coef[n, block(i)] for n in range(6)], (0, 5), force
        )

    changes = []
    for c in range(2):
        for q in range(2):
            w01[c, q, 0:12] = a01_ref[c, q, 48:60, 0:256]
            w01[c, q, 12:24] = a01_ref[c, q, 48:60, 256:512]
            changes.append(series[2 * m + c, q, 8:32] - w01[c, q])
    for q in range(2):
        changes.append(series[2 * m + 2, q, 12:28] - w2_ref[q])
    refined = exact_dot(jnp.concatenate(changes, axis=0), up_matrix(512))
    for c in range(2):
        for q in range(2):
            n = 2 * c + q
            fine[0, c, q] = a01_ref[c, q, 0:48] + rows.repeat(refined[24 * n : 24 * n + 24])
    for q in range(2):
        out_ref[15, q] = a2_ref[q] + rows.repeat(refined[96 + 16 * q : 112 + 16 * q])
        out_ref[7, q] = fine[0, 1, q, 8:40]

    def leave(n):
        return pltpu.make_async_copy(out_ref.at[n], result_ref.at[n], sems.at[n])

    leave(15).start()
    leave(7).start()

    def fine_step(source, target, position):
        for c in range(2):

            def load(i):
                return [fine[source, c, q, block(i)] for q in range(2)]

            def store(i, values):
                for q in range(2):
                    fine[target, c, q, block(i)] = values[q]
                    if 1 <= i < 5:
                        out_ref[8 * c + position, q, block(i - 1)] = values[q]

            advance(load, store, lambda i: [fine_ref[n, block(i)] for n in range(6)], (0, 6))
            leave(8 * c + position).start()

    def pair(n, carry):
        fine_step(0, 1, 2 * n)
        fine_step(1, 0, 2 * n + 1)
        return carry

    lax.fori_loop(0, 3, pair, 0)
    fine_step(0, 1, 6)
    for n in range(16):
        leave(n).wait()


def struct(*shape):
    return jax.ShapeDtypeStruct(shape, F32)


def scratch(*shape):
    return pltpu.VMEM(shape, F32)


def device(t, s):
    return t * N_SPACE + s


def send(x, dt, ds):
    pairs = [
        (device(t, s), device((t + dt) % N_TM, s + ds))
        for t in range(N_TM)
        for s in range(N_SPACE)
        if 0 <= s + ds < N_SPACE
    ]
    return lax.ppermute(x, AXES, pairs)


def from_group_behind(x, ds):
    pairs = []
    for k in range(GROUP):
        for m in range(k):
            for s in range(N_SPACE):
                if 0 <= s + ds < N_SPACE:
                    pairs.append((device(4 * (k - 1 - m) + m, s + ds), device(4 * k + m, s)))
    return lax.ppermute(x, AXES, pairs)


def local(initial, guess, kappa, feed, kill, react):
    k, m = lax.axis_index("k"), lax.axis_index("m")
    where = jnp.stack([GROUP * k + m, k, m]).astype(jnp.int32)
    own, low_edge, high_edge = pl.pallas_call(
        pack_kernel,
        out_shape=(struct(9, 32, 512), struct(9, 16, 512), struct(9, 16, 512)),
        in_specs=[SMEM] + [ANY] * 6,
        out_specs=(VMEM,) * 3,
        scratch_shapes=[pltpu.SemaphoreType.DMA((18,))],
    )(where, initial, guess, kappa, feed, kill, react)
    lo = send(low_edge, 0, 1)
    hi = send(high_edge, 0, -1)
    a01, a2, w2, held, packed, fine = pl.pallas_call(
        fine_kernel,
        out_shape=(
            struct(2, 2, 60, 512), struct(2, 32, 512), struct(2, 16, 256),
            struct(6, 16, 256), struct(11, 16, 256), struct(6, 48, 512),
        ),
        in_specs=[SMEM] + [VMEM] * 3,
        out_specs=(VMEM,) * 6,
        scratch_shapes=[
            scratch(2, 2, 64, 512), scratch(2, 2, 64, 512), scratch(5, 64, 512),
            scratch(6, 64, 512), scratch(2, 2, 32, 256), scratch(6, 32, 256),
            scratch(60, 64, 128),
        ],
    )(where, own, lo, hi)
    lo = send(packed, 1, 1)
    hi = send(packed, 1, -1)
    middle = send(held, 1, 0)
    window = jnp.concatenate([lo[:6, 4:], middle, hi[:6, :12]], axis=1)
    gathered = lax.all_gather(window, "m", axis=0, tiled=False)
    gathered, a01 = lax.optimization_barrier((gathered, a01))
    a01 = send(a01, 1, 0)
    pred, mid_coef = pl.pallas_call(
        mid_kernel,
        out_shape=(struct(4, 8, 128), struct(6, 40, 256)),
        in_specs=[VMEM] * 4,
        out_specs=(VMEM,) * 2,
        scratch_shapes=[scratch(5, 48, 256), scratch(2, 2, 40, 256), scratch(8, 16, 128)],
    )(gathered, packed, lo, hi)
    pieces = [from_group_behind(pred, ds) for ds in (-1, 0, 1)]
    top = lax.all_gather(jnp.stack(pieces), "m", axis=0, tiled=False)
    return pl.pallas_call(
        final_kernel,
        out_shape=struct(16, 2, 32, 512),
        in_specs=[SMEM] + [VMEM] * 11,
        out_specs=ANY,
        scratch_shapes=[
            scratch(5, 48, 256), scratch(6, 24, 128), scratch(4, 2, 24, 128),
            scratch(9, 2, 40, 256), scratch(50, 48, 128), scratch(2, 2, 2, 48, 512),
            scratch(2, 2, 24, 256), scratch(16, 2, 32, 512), pltpu.SemaphoreType.DMA((16,)),
        ],
    )(where, gathered, top, pred, mid_coef, packed, lo, hi, a01, a2, w2, fine)


def solution(mesh):
    split = Mesh(mesh.devices.reshape(4, 4, 16), AXES)
    tm = ("k", "m")
    placed = (
        P(None, "space", None),
        P(tm, None, "space", None),
        P(None, "space", None),
        P("space", None),
        P("space", None),
        P("space", None),
    )
    return jax.shard_map(
        local, mesh=split, in_specs=placed, out_specs=P(tm, None, "space", None), check_vma=False
    )
```

```python
import jax
import jax.numpy as jnp
from jax import lax
from jax.experimental import pallas as pl
from jax.experimental.pallas import tpu as pltpu
from jax.sharding import Mesh
from jax.sharding import PartitionSpec as P

F32 = jnp.float32
AXES = ("k", "m", "space")
VMEM = pl.BlockSpec(memory_space=pltpu.VMEM)
HBM = pl.BlockSpec(memory_space=pltpu.HBM)
N_TM = 16
N_SPACE = 16
GROUP = 4
STRIP = 32


def exact_dot(x, matrix):
    high = x.astype(jnp.bfloat16)
    rest = x - high.astype(F32)
    middle = rest.astype(jnp.bfloat16)
    low = (rest - middle.astype(F32)).astype(jnp.bfloat16)

    def part(piece):
        return lax.dot_general(
            piece, matrix, (((1,), (0,)), ((), ())), preferred_element_type=F32
        )

    return part(low) + part(middle) + part(high)


def down_matrix(fine):
    rows = lax.broadcasted_iota(jnp.int32, (fine, fine // 2), 0)
    cols = lax.broadcasted_iota(jnp.int32, (fine, fine // 2), 1)
    inside = (rows == 2 * cols) | (rows == 2 * cols + 1)
    return jnp.where(inside, F32(0.25), F32(0.0)).astype(jnp.bfloat16)


def up_matrix(fine):
    rows = lax.broadcasted_iota(jnp.int32, (fine // 2, fine), 0)
    cols = lax.broadcasted_iota(jnp.int32, (fine // 2, fine), 1)
    inside = (cols == 2 * rows) | (cols == 2 * rows + 1)
    return jnp.where(inside, F32(1.0), F32(0.0)).astype(jnp.bfloat16)


def split_tiles(x):
    return [x[:, 128 * k : 128 * k + 128] for k in range(x.shape[1] // 128)]


def side_sums(tiles, lane_first, lane_last):
    right_going = [pltpu.roll(t, 1, 1) for t in tiles]
    left_going = [pltpu.roll(t, 127, 1) for t in tiles]
    zero = jnp.zeros_like(tiles[0])
    out = []
    for k in range(len(tiles)):
        before = right_going[k - 1] if k > 0 else zero
        after = left_going[k + 1] if k < len(tiles) - 1 else zero
        out.append(
            jnp.where(lane_first, before, right_going[k])
            + jnp.where(lane_last, after, left_going[k])
        )
    return out


def advance(load, store, coeffs, blocks, force=None):
    sub = lax.broadcasted_iota(jnp.int32, (8, 128), 0)
    lane = lax.broadcasted_iota(jnp.int32, (8, 128), 1)
    first_row, last_row = sub == 0, sub == 7
    first_lane, last_lane = lane == 0, lane == 127
    held = {}

    def fetch(i):
        if i not in held:
            species = []
            for x in load(i):
                tiles = split_tiles(x)
                species.append(
                    (
                        tiles,
                        [pltpu.roll(t, 1, 0) for t in tiles],
                        [pltpu.roll(t, 7, 0) for t in tiles],
                    )
                )
            held[i] = species
        return held[i]

    low, high = blocks
    for i in range(low, high):
        here = fetch(i)
        above = fetch(max(i - 1, low))
        below = fetch(min(i + 1, high - 1))
        held.pop(i - 2, None)
        c = coeffs(i)
        sums = []
        for q in range(2):
            tiles, down, up = here[q]
            sides = side_sums(tiles, first_lane, last_lane)
            sums.append(
                [
                    jnp.where(first_row, above[q][1][k], down[k])
                    + jnp.where(last_row, below[q][2][k], up[k])
                    + sides[k]
                    for k in range(len(tiles))
                ]
            )
        next_a, next_b = [], []
        spread_a, spread_b, supply, keep_a, keep_b, coupling = [split_tiles(x) for x in c]
        for k in range(len(sums[0])):
            a, b = here[0][0][k], here[1][0][k]
            coupled = coupling[k] * a * b * b
            next_a.append(keep_a[k] * a + spread_a[k] * sums[0][k] + (supply[k] - coupled))
            next_b.append(keep_b[k] * b + spread_b[k] * sums[1][k] + coupled)
        out = [jnp.concatenate(next_a, axis=1), jnp.concatenate(next_b, axis=1)]
        if force is not None:
            extra = force(i)
            out = [out[0] + extra[0], out[1] + extra[1]]
        store(i, out)


def advanced(values, coeffs, force=None):
    out = [None] * len(values)

    def store(i, new):
        out[i] = new

    advance(lambda i: values[i], store, coeffs, (0, len(values)), force)
    return out


def derived(spread_a, spread_b, supply, removal, coupling):
    return (
        spread_a,
        spread_b,
        supply,
        1.0 - supply - 4.0 * spread_a,
        1.0 - supply - removal - 4.0 * spread_b,
        coupling,
    )


def block(i):
    return slice(8 * i, 8 * i + 8)


class Rows:
    def __init__(self, ref):
        self.ref, self.used = ref, 0

    def coarsen(self, x):
        count = x.shape[0]
        parts = []
        for tile in split_tiles(x):
            n = self.used
            self.used += 1
            self.ref[n, 0:count] = tile
            even = self.ref[n, pl.ds(0, count // 2, stride=2)]
            parts.append(even + self.ref[n, pl.ds(1, count // 2, stride=2)])
        return jnp.concatenate(parts, axis=1)

    def repeat(self, x):
        count = x.shape[0]
        parts = []
        for tile in split_tiles(x):
            n = self.used
            self.used += 1
            self.ref[n, pl.ds(0, count, stride=2)] = tile
            self.ref[n, pl.ds(1, count, stride=2)] = tile
            parts.append(self.ref[n, 0 : 2 * count])
        return jnp.concatenate(parts, axis=1)


def pack_kernel(
    initial_ref, guess_ref, kappa_ref, feed_ref, kill_ref, react_ref,
    own_ref, low_ref, high_ref, sems,
):
    last = GROUP * lax.axis_index("k") + lax.axis_index("m") == N_TM - 1
    count = [0]

    def copy(source, target):
        n = count[0]
        count[0] += 1
        return pltpu.make_async_copy(source, target, sems.at[n])

    def copies(pick, place, many):
        out = []
        at = pl.ds(place, many) if many > 1 else place
        for target, low, size in ((own_ref, 0, 32), (low_ref, 16, 16), (high_ref, 0, 16)):
            out.append(copy(pick(pl.ds(low, size)), target.at[at]))
        return out

    plain = []
    plain += copies(lambda r: guess_ref.at[7, :, r], 5, 2)
    plain += copies(lambda r: kappa_ref.at[:, r], 0, 2)
    plain += copies(lambda r: feed_ref.at[r], 2, 1)
    plain += copies(lambda r: kill_ref.at[r], 3, 1)
    plain += copies(lambda r: react_ref.at[r], 4, 1)
    for c in plain:
        c.start()
    mark = count[0]
    ends = copies(lambda r: guess_ref.at[15, :, r], 7, 2)
    count[0] = mark
    starts = copies(lambda r: initial_ref.at[:, r], 7, 2)

    @pl.when(last)
    def _():
        for c in starts:
            c.start()

    @pl.when(jnp.logical_not(last))
    def _():
        for c in ends:
            c.start()

    for c in plain + ends:
        c.wait()


def fine_kernel(
    own_ref, lo_ref, hi_ref,
    a01_ref, a2_ref, w2_ref, packed_ref, send_ref, fine_ref,
    s0, s1, raw, tall, mid_state, mid_coef, cells,
):
    rows = Rows(cells)
    last = GROUP * lax.axis_index("k") + lax.axis_index("m") == N_TM - 1
    for c in range(2):
        for q in range(2):
            f = 5 + 2 * c + q
            s0[c, q, 0:16] = lo_ref[f]
            s0[c, q, 16:48] = own_ref[f]
            s0[c, q, 48:64] = hi_ref[f]
    for f in range(5):
        raw[f, 0:16] = lo_ref[f]
        raw[f, 16:48] = own_ref[f]
        raw[f, 48:64] = hi_ref[f]
    for i in range(8):
        r = block(i)
        parts = derived(*[raw[f, r] for f in range(5)])
        for n in range(6):
            tall[n, r] = parts[n]
        if 1 <= i < 7:
            for n in range(6):
                fine_ref[n, block(i - 1)] = parts[n]

    def coeffs(i):
        return [tall[n, block(i)] for n in range(6)]

    def run(source, target, chain, blocks):
        def load(i):
            return [source[chain, q, block(i)] for q in range(2)]

        def store(i, values):
            for q in range(2):
                target[chain, q, block(i)] = values[q]

        advance(load, store, coeffs, blocks)

    def first_pair(n, carry):
        for source, target in ((s0, s1), (s1, s0)):
            run(source, target, 0, (0, 8))
            run(source, target, 1, (0, 8))
        return carry

    lax.fori_loop(0, 4, first_pair, 0)

    for q in range(2):
        a2_ref[q] = s0[0, q, 16:48]
    stacked = [rows.coarsen(s0[0, q, 16:48]) for q in range(2)]
    for q in range(2):
        s0[0, q, 0:16] = jnp.where(last, lo_ref[7 + q], s0[0, q, 0:16])
        s0[0, q, 16:48] = jnp.where(last, own_ref[7 + q], s0[0, q, 16:48])
        s0[0, q, 48:64] = jnp.where(last, hi_ref[7 + q], s0[0, q, 48:64])
    for q in range(2):
        for c in range(2):
            a01_ref[c, q, 0:48] = s0[c, q, 8:56]

    stacked += [rows.coarsen(raw[f]) for f in range(5)]
    stacked += [rows.coarsen(s0[c, q]) for c in range(2) for q in range(2)]
    down = down_matrix(512)
    coarse = exact_dot(jnp.concatenate(stacked, axis=0), down)
    for q in range(2):
        w2_ref[q] = coarse[16 * q : 16 * q + 16]
    base = 32
    for f in range(5):
        send_ref[6 + f] = coarse[base + 32 * f + 8 : base + 32 * f + 24]
    for i in range(4):
        at = [coarse[base + 32 * f + 8 * i : base + 32 * f + 8 * i + 8] for f in range(5)]
        parts = derived(2.0 * at[0], 2.0 * at[1], 8.0 * at[2], 8.0 * at[3], 8.0 * at[4])
        for n in range(6):
            mid_coef[n, block(i)] = parts[n]
    base = 192
    for c in range(2):
        for q in range(2):
            n = base + 32 * (2 * c + q)
            mid_state[c, q] = coarse[n : n + 32]
            a01_ref[c, q, 48:60, 0:256] = coarse[n + 4 : n + 16]
            a01_ref[c, q, 48:60, 256:512] = coarse[n + 16 : n + 28]
    for q in range(2):
        send_ref[4 + q] = mid_state[0, q, 8:24]
        packed_ref[4 + q] = mid_state[0, q, 8:24]

    def second_pair(n, carry):
        for source, target in ((s0, s1), (s1, s0)):
            run(source, target, 0, (1, 7))
            run(source, target, 1, (1, 7))
        return carry

    lax.fori_loop(0, 4, second_pair, 0)

    stacked = jnp.concatenate(
        [rows.coarsen(s0[c, q, 16:48]) for c in range(2) for q in range(2)], axis=0
    )
    coarse = exact_dot(stacked, down)
    for c in range(2):

        def load(i):
            return [mid_state[c, q, block(i)] for q in range(2)]

        def store(i, values):
            if 1 <= i < 3:
                for q in range(2):
                    n = 16 * (2 * c + q) + 8 * (i - 1)
                    forcing = coarse[n : n + 8] - values[q]
                    send_ref[2 * c + q, block(i - 1)] = forcing
                    packed_ref[2 * c + q, block(i - 1)] = forcing

        advance(load, store, lambda i: [mid_coef[n, block(i)] for n in range(6)], (0, 4))


def wide_mid_coefs(raw, coef_ref, lo_ref, hi_ref, mid_coef):
    for f in range(5):
        raw[f, 0:16] = lo_ref[6 + f]
        raw[f, 16:32] = coef_ref[6 + f]
        raw[f, 32:48] = hi_ref[6 + f]
    at = [raw[f, 4:44] for f in range(5)]
    parts = derived(2.0 * at[0], 2.0 * at[1], 8.0 * at[2], 8.0 * at[3], 8.0 * at[4])
    for n in range(6):
        mid_coef[n] = parts[n]


def mid_kernel(
    gathered_ref, own_ref, lo_ref, hi_ref, out_ref, coef_out_ref, raw, state, cells,
):
    rows = Rows(cells)
    wide_mid_coefs(raw, own_ref, lo_ref, hi_ref, coef_out_ref)

    def coeffs(i):
        return [coef_out_ref[n, block(i)] for n in range(6)]

    values = [[gathered_ref[0, 4 + q, block(i)] for q in range(2)] for i in range(5)]
    for step in range(8):
        holder, place = step // 2, step % 2

        def force(i):
            return [gathered_ref[holder, 2 * place + q, block(i)] for q in range(2)]

        values = advanced(values, coeffs, force)
    for i in range(5):
        for q in range(2):
            state[q, block(i)] = values[i][q]
    stacked = jnp.concatenate(
        [rows.coarsen(state[q, 12:28]) for q in range(2)]
        + [rows.coarsen(gathered_ref[0, 4 + q, 12:28]) for q in range(2)],
        axis=0,
    )
    coarse = exact_dot(stacked, down_matrix(256))
    for f in range(4):
        out_ref[f] = coarse[8 * f : 8 * f + 8]


def final_kernel(
    gathered_ref, top_ref, pred_ref, mid_coef, own_ref, lo_ref, hi_ref,
    a01_ref, a2_ref, w2_ref, fine_ref,
    result_ref,
    raw, low_coef, yz, series, cells, fine, w01, out_ref, sems,
):
    rows = Rows(cells)
    k, m = lax.axis_index("k"), lax.axis_index("m")
    for f in range(5):
        raw[f, 0:16] = lo_ref[6 + f]
        raw[f, 16:32] = own_ref[6 + f]
        raw[f, 32:48] = hi_ref[6 + f]
    down = down_matrix(256)
    up_low = up_matrix(256)
    stacked = jnp.concatenate([rows.coarsen(raw[f]) for f in range(5)], axis=0)
    coarse = exact_dot(stacked, down)
    at = [coarse[24 * f : 24 * f + 24] for f in range(5)]
    parts = derived(4.0 * at[0], 4.0 * at[1], 64.0 * at[2], 64.0 * at[3], 64.0 * at[4])
    for n in range(6):
        low_coef[n] = parts[n]

    def low_step(values):
        return advanced(values, lambda i: [low_coef[n, block(i)] for n in range(6)])

    def kept(slot):
        return [[yz[slot, q, block(i)] for q in range(2)] for i in range(3)]

    values = [[top_ref[2, i, q] for q in range(2)] for i in range(3)]
    for back in (1, 0):
        follows = jnp.where(k - 1 - back > 0, F32(1.0), F32(0.0))
        other = low_step([[top_ref[back, i, 2 + q] for q in range(2)] for i in range(3)])
        values = low_step(values)
        values = [
            [top_ref[back, i, q] + follows * (values[i][q] - other[i][q]) for q in range(2)]
            for i in range(3)
        ]
    for i in range(3):
        for q in range(2):
            yz[0, q, block(i)] = values[i][q]
    stacked = jnp.concatenate(
        [rows.coarsen(gathered_ref[0, 4 + q]) for q in range(2)]
        + [rows.coarsen(w2_ref[q]) for q in range(2)]
        + [jnp.zeros((8, 256), F32)],
        axis=0,
    )
    coarse = exact_dot(stacked, down)
    inner = jnp.where(k > 0, F32(1.0), F32(0.0))
    fixes = []
    for q in range(2):
        z = coarse[20 * q : 20 * q + 20]
        yz[1, q] = jnp.zeros((24, 128), F32)
        yz[1, q, 2:22] = z
        fixes.append(inner * (yz[0, q, 2:22] - z))
    values, other = low_step(values), low_step(kept(1))
    for q in range(2):
        end = pred_ref[q] + inner * (values[1][q] - other[1][q])
        fixes.append(end - coarse[40 + 8 * q : 48 + 8 * q])
    fixes.append(jnp.zeros((8, 128), F32))
    refined = exact_dot(jnp.concatenate(fixes, axis=0), up_low)
    for q in range(2):
        series[0, q] = gathered_ref[0, 4 + q] + rows.repeat(refined[20 * q : 20 * q + 20])
        end = rows.repeat(refined[40 + 8 * q : 48 + 8 * q])
        series[8, q, 12:28] = w2_ref[q] + end

    values = [[series[0, q, block(i)] for q in range(2)] for i in range(5)]
    for step in range(7):
        holder, place = step // 2, step % 2

        def force(i):
            return [gathered_ref[holder, 2 * place + q, block(i)] for q in range(2)]

        values = advanced(values, lambda i: [mid_coef[n, block(i)] for n in range(6)], force)
        for i in range(5):
            for q in range(2):
                series[step + 1, q, block(i)] = values[i][q]

    changes = []
    for c in range(2):
        for q in range(2):
            w01[c, q, 0:12] = a01_ref[c, q, 48:60, 0:256]
            w01[c, q, 12:24] = a01_ref[c, q, 48:60, 256:512]
            changes.append(series[2 * m + c, q, 8:32] - w01[c, q])
    for q in range(2):
        changes.append(series[2 * m + 2, q, 12:28] - w2_ref[q])
    refined = exact_dot(jnp.concatenate(changes, axis=0), up_matrix(512))
    for c in range(2):
        for q in range(2):
            n = 2 * c + q
            fine[0, c, q] = a01_ref[c, q, 0:48] + rows.repeat(refined[24 * n : 24 * n + 24])
    for q in range(2):
        out_ref[15, q] = a2_ref[q] + rows.repeat(refined[96 + 16 * q : 112 + 16 * q])
        out_ref[7, q] = fine[0, 1, q, 8:40]

    def leave(n):
        return pltpu.make_async_copy(out_ref.at[n], result_ref.at[n], sems.at[n])

    leave(15).start()
    leave(7).start()

    def fine_step(source, target, position):
        for c in range(2):

            def load(i):
                return [fine[source, c, q, block(i)] for q in range(2)]

            def store(i, values):
                for q in range(2):
                    fine[target, c, q, block(i)] = values[q]
                    if 1 <= i < 5:
                        out_ref[8 * c + position, q, block(i - 1)] = values[q]

            advance(load, store, lambda i: [fine_ref[n, block(i)] for n in range(6)], (0, 6))
            leave(8 * c + position).start()

    def pair(n, carry):
        fine_step(0, 1, 2 * n)
        fine_step(1, 0, 2 * n + 1)
        return carry

    lax.fori_loop(0, 3, pair, 0)
    fine_step(0, 1, 6)
    for n in range(16):
        leave(n).wait()


def struct(*shape):
    return pltpu.VMEM(shape, F32)


def scratch(*shape):
    return pltpu.VMEM(shape, F32)


def limit(mib):
    return pltpu.CompilerParams(vmem_limit_bytes=mib * 2**20)


def near(x):
    return pltpu.with_memory_space_constraint(x, pltpu.VMEM)


def far(x):
    return pltpu.with_memory_space_constraint(x, pltpu.HBM)


def device(t, s):
    return t * N_SPACE + s


def send(x, dt, ds):
    pairs = [
        (device(t, s), device((t + dt) % N_TM, s + ds))
        for t in range(N_TM)
        for s in range(N_SPACE)
        if 0 <= s + ds < N_SPACE
    ]
    return lax.ppermute(x, AXES, pairs)


def from_group_behind(x, ds):
    pairs = []
    for k in range(GROUP):
        for m in range(k):
            for s in range(N_SPACE):
                if 0 <= s + ds < N_SPACE:
                    pairs.append((device(4 * (k - 1 - m) + m, s + ds), device(4 * k + m, s)))
    return lax.ppermute(x, AXES, pairs)


def local(initial, guess, kappa, feed, kill, react):
    own, low_edge, high_edge = pl.pallas_call(
        pack_kernel,
        out_shape=(struct(9, 32, 512), struct(9, 16, 512), struct(9, 16, 512)),
        in_specs=[HBM] * 6,
        out_specs=(VMEM,) * 3,
        scratch_shapes=[pltpu.SemaphoreType.DMA((18,))],
        compiler_params=limit(4),
    )(*[far(x) for x in (initial, guess, kappa, feed, kill, react)])
    lo = send(low_edge, 0, 1)
    hi = send(high_edge, 0, -1)
    a01, a2, w2, held, packed, fine = pl.pallas_call(
        fine_kernel,
        out_shape=(
            struct(2, 2, 60, 512), struct(2, 32, 512), struct(2, 16, 256),
            struct(6, 16, 256), struct(11, 16, 256), struct(6, 48, 512),
        ),
        in_specs=[VMEM] * 3,
        out_specs=(VMEM,) * 6,
        scratch_shapes=[
            scratch(2, 2, 64, 512), scratch(2, 2, 64, 512), scratch(5, 64, 512),
            scratch(6, 64, 512), scratch(2, 2, 32, 256), scratch(6, 32, 256),
            scratch(60, 64, 128),
        ],
        compiler_params=limit(14),
    )(near(own), near(lo), near(hi))
    lo = send(packed, 1, 1)
    hi = send(packed, 1, -1)
    middle = send(held, 1, 0)
    window = jnp.concatenate([lo[:6, 4:], middle, hi[:6, :12]], axis=1)
    gathered = lax.all_gather(window, "m", axis=0, tiled=False)
    gathered, a01 = lax.optimization_barrier((gathered, a01))
    a01 = send(a01, 1, 0)
    pred, mid_coef = pl.pallas_call(
        mid_kernel,
        out_shape=(struct(4, 8, 128), struct(6, 40, 256)),
        in_specs=[VMEM] * 4,
        out_specs=(VMEM,) * 2,
        scratch_shapes=[scratch(5, 48, 256), scratch(2, 40, 256), scratch(8, 16, 128)],
        compiler_params=limit(8),
    )(near(gathered), near(packed), near(lo), near(hi))
    pieces = [from_group_behind(pred, ds) for ds in (-1, 0, 1)]
    top = lax.all_gather(jnp.stack(pieces), "m", axis=0, tiled=False)
    return pl.pallas_call(
        final_kernel,
        out_shape=jax.ShapeDtypeStruct((16, 2, 32, 512), F32),
        in_specs=[VMEM] * 11,
        out_specs=HBM,
        scratch_shapes=[
            scratch(5, 48, 256), scratch(6, 24, 128), scratch(2, 2, 24, 128),
            scratch(9, 2, 40, 256), scratch(50, 48, 128), scratch(2, 2, 2, 48, 512),
            scratch(2, 2, 24, 256), scratch(16, 2, 32, 512), pltpu.SemaphoreType.DMA((16,)),
        ],
        compiler_params=limit(18),
    )(*[near(x) for x in (gathered, top, pred, mid_coef, packed, lo, hi, a01, a2, w2, fine)])


def solution(mesh):
    split = Mesh(mesh.devices.reshape(4, 4, 16), AXES)
    tm = ("k", "m")
    placed = (
        P(None, "space", None),
        P(tm, None, "space", None),
        P(None, "space", None),
        P("space", None),
        P("space", None),
        P("space", None),
    )
    return jax.shard_map(
        local, mesh=split, in_specs=placed, out_specs=P(tm, None, "space", None), check_vma=False
    )
```

```python
import jax
import jax.numpy as jnp
from jax import lax
from jax.experimental import pallas as pl
from jax.experimental.pallas import tpu as pltpu
from jax.sharding import Mesh
from jax.sharding import PartitionSpec as P

F32 = jnp.float32
AXES = ("k", "m", "space")
VMEM = pl.BlockSpec(memory_space=pltpu.VMEM)
HBM = pl.BlockSpec(memory_space=pltpu.HBM)
N_TM = 16
N_SPACE = 16
GROUP = 4
STRIP = 32


def exact_dot(x, matrix):
    high = x.astype(jnp.bfloat16)
    rest = x - high.astype(F32)
    middle = rest.astype(jnp.bfloat16)
    low = (rest - middle.astype(F32)).astype(jnp.bfloat16)

    def part(piece):
        return lax.dot_general(
            piece, matrix, (((1,), (0,)), ((), ())), preferred_element_type=F32
        )

    return part(low) + part(middle) + part(high)


def down_matrix(fine):
    rows = lax.broadcasted_iota(jnp.int32, (fine, fine // 2), 0)
    cols = lax.broadcasted_iota(jnp.int32, (fine, fine // 2), 1)
    inside = (rows == 2 * cols) | (rows == 2 * cols + 1)
    return jnp.where(inside, F32(0.25), F32(0.0)).astype(jnp.bfloat16)


def up_matrix(fine):
    rows = lax.broadcasted_iota(jnp.int32, (fine // 2, fine), 0)
    cols = lax.broadcasted_iota(jnp.int32, (fine // 2, fine), 1)
    inside = (cols == 2 * rows) | (cols == 2 * rows + 1)
    return jnp.where(inside, F32(1.0), F32(0.0)).astype(jnp.bfloat16)


def split_tiles(x):
    return [x[:, 128 * k : 128 * k + 128] for k in range(x.shape[1] // 128)]


def side_sums(tiles, lane_first, lane_last):
    right_going = [pltpu.roll(t, 1, 1) for t in tiles]
    left_going = [pltpu.roll(t, 127, 1) for t in tiles]
    zero = jnp.zeros_like(tiles[0])
    out = []
    for k in range(len(tiles)):
        before = right_going[k - 1] if k > 0 else zero
        after = left_going[k + 1] if k < len(tiles) - 1 else zero
        out.append(
            jnp.where(lane_first, before, right_going[k])
            + jnp.where(lane_last, after, left_going[k])
        )
    return out


def advance(load, store, coeffs, blocks, force=None):
    sub = lax.broadcasted_iota(jnp.int32, (8, 128), 0)
    lane = lax.broadcasted_iota(jnp.int32, (8, 128), 1)
    first_row, last_row = sub == 0, sub == 7
    first_lane, last_lane = lane == 0, lane == 127
    held = {}

    def fetch(i):
        if i not in held:
            species = []
            for x in load(i):
                tiles = split_tiles(x)
                species.append(
                    (
                        tiles,
                        [pltpu.roll(t, 1, 0) for t in tiles],
                        [pltpu.roll(t, 7, 0) for t in tiles],
                    )
                )
            held[i] = species
        return held[i]

    low, high = blocks
    for i in range(low, high):
        here = fetch(i)
        above = fetch(max(i - 1, low))
        below = fetch(min(i + 1, high - 1))
        held.pop(i - 2, None)
        c = coeffs(i)
        sums = []
        for q in range(2):
            tiles, down, up = here[q]
            sides = side_sums(tiles, first_lane, last_lane)
            sums.append(
                [
                    jnp.where(first_row, above[q][1][k], down[k])
                    + jnp.where(last_row, below[q][2][k], up[k])
                    + sides[k]
                    for k in range(len(tiles))
                ]
            )
        next_a, next_b = [], []
        spread_a, spread_b, supply, keep_a, keep_b, coupling = [split_tiles(x) for x in c]
        for k in range(len(sums[0])):
            a, b = here[0][0][k], here[1][0][k]
            coupled = coupling[k] * a * b * b
            next_a.append(keep_a[k] * a + spread_a[k] * sums[0][k] + (supply[k] - coupled))
            next_b.append(keep_b[k] * b + spread_b[k] * sums[1][k] + coupled)
        out = [jnp.concatenate(next_a, axis=1), jnp.concatenate(next_b, axis=1)]
        if force is not None:
            extra = force(i)
            out = [out[0] + extra[0], out[1] + extra[1]]
        store(i, out)


def advanced(values, coeffs, force=None):
    out = [None] * len(values)

    def store(i, new):
        out[i] = new

    advance(lambda i: values[i], store, coeffs, (0, len(values)), force)
    return out


def derived(spread_a, spread_b, supply, removal, coupling):
    return (
        spread_a,
        spread_b,
        supply,
        1.0 - supply - 4.0 * spread_a,
        1.0 - supply - removal - 4.0 * spread_b,
        coupling,
    )


def block(i):
    return slice(8 * i, 8 * i + 8)


class Rows:
    def __init__(self, ref):
        self.ref, self.used = ref, 0

    def coarsen(self, x):
        count = x.shape[0]
        parts = []
        for tile in split_tiles(x):
            n = self.used
            self.used += 1
            self.ref[n, 0:count] = tile
            even = self.ref[n, pl.ds(0, count // 2, stride=2)]
            parts.append(even + self.ref[n, pl.ds(1, count // 2, stride=2)])
        return jnp.concatenate(parts, axis=1)

    def repeat(self, x):
        count = x.shape[0]
        parts = []
        for tile in split_tiles(x):
            n = self.used
            self.used += 1
            self.ref[n, pl.ds(0, count, stride=2)] = tile
            self.ref[n, pl.ds(1, count, stride=2)] = tile
            parts.append(self.ref[n, 0 : 2 * count])
        return jnp.concatenate(parts, axis=1)


def pack_kernel(
    initial_ref, guess_ref, kappa_ref, feed_ref, kill_ref, react_ref,
    own_ref, low_ref, high_ref, sems,
):
    last = GROUP * lax.axis_index("k") + lax.axis_index("m") == N_TM - 1
    count = [0]

    def copy(source, target):
        n = count[0]
        count[0] += 1
        return pltpu.make_async_copy(source, target, sems.at[n])

    def copies(pick, place, many):
        out = []
        at = pl.ds(place, many) if many > 1 else place
        for target, low, size in ((own_ref, 0, 32), (low_ref, 16, 16), (high_ref, 0, 16)):
            out.append(copy(pick(pl.ds(low, size)), target.at[at]))
        return out

    plain = []
    plain += copies(lambda r: guess_ref.at[7, :, r], 5, 2)
    plain += copies(lambda r: kappa_ref.at[:, r], 0, 2)
    plain += copies(lambda r: feed_ref.at[r], 2, 1)
    plain += copies(lambda r: kill_ref.at[r], 3, 1)
    plain += copies(lambda r: react_ref.at[r], 4, 1)
    for c in plain:
        c.start()
    mark = count[0]
    ends = copies(lambda r: guess_ref.at[15, :, r], 7, 2)
    count[0] = mark
    starts = copies(lambda r: initial_ref.at[:, r], 7, 2)

    @pl.when(last)
    def _():
        for c in starts:
            c.start()

    @pl.when(jnp.logical_not(last))
    def _():
        for c in ends:
            c.start()

    for c in plain + ends:
        c.wait()


def fine_kernel(
    own_ref, lo_ref, hi_ref,
    a01_ref, a2_ref, w2_ref, packed_ref, send_ref, fine_ref,
    s0, s1, raw, tall, mid_state, mid_coef, cells,
):
    rows = Rows(cells)
    last = GROUP * lax.axis_index("k") + lax.axis_index("m") == N_TM - 1
    for c in range(2):
        for q in range(2):
            f = 5 + 2 * c + q
            s0[c, q, 0:16] = lo_ref[f]
            s0[c, q, 16:48] = own_ref[f]
            s0[c, q, 48:64] = hi_ref[f]
    for f in range(5):
        raw[f, 0:16] = lo_ref[f]
        raw[f, 16:48] = own_ref[f]
        raw[f, 48:64] = hi_ref[f]
    for i in range(8):
        r = block(i)
        parts = derived(*[raw[f, r] for f in range(5)])
        for n in range(6):
            tall[n, r] = parts[n]
        if 1 <= i < 7:
            for n in range(6):
                fine_ref[n, block(i - 1)] = parts[n]

    def coeffs(i):
        return [tall[n, block(i)] for n in range(6)]

    def run(source, target, chain, blocks):
        def load(i):
            return [source[chain, q, block(i)] for q in range(2)]

        def store(i, values):
            for q in range(2):
                target[chain, q, block(i)] = values[q]

        advance(load, store, coeffs, blocks)

    def first_pair(n, carry):
        for source, target in ((s0, s1), (s1, s0)):
            run(source, target, 0, (0, 8))
            run(source, target, 1, (0, 8))
        return carry

    lax.fori_loop(0, 4, first_pair, 0)

    for q in range(2):
        a2_ref[q] = s0[0, q, 16:48]
    stacked = [rows.coarsen(s0[0, q, 16:48]) for q in range(2)]
    for q in range(2):
        s0[0, q, 0:16] = jnp.where(last, lo_ref[7 + q], s0[0, q, 0:16])
        s0[0, q, 16:48] = jnp.where(last, own_ref[7 + q], s0[0, q, 16:48])
        s0[0, q, 48:64] = jnp.where(last, hi_ref[7 + q], s0[0, q, 48:64])
    for q in range(2):
        for c in range(2):
            a01_ref[c, q, 0:48] = s0[c, q, 8:56]

    stacked += [rows.coarsen(raw[f]) for f in range(5)]
    stacked += [rows.coarsen(s0[c, q]) for c in range(2) for q in range(2)]
    down = down_matrix(512)
    coarse = exact_dot(jnp.concatenate(stacked, axis=0), down)
    for q in range(2):
        w2_ref[q] = coarse[16 * q : 16 * q + 16]
    base = 32
    for f in range(5):
        send_ref[6 + f] = coarse[base + 32 * f + 8 : base + 32 * f + 24]
    for i in range(4):
        at = [coarse[base + 32 * f + 8 * i : base + 32 * f + 8 * i + 8] for f in range(5)]
        parts = derived(2.0 * at[0], 2.0 * at[1], 8.0 * at[2], 8.0 * at[3], 8.0 * at[4])
        for n in range(6):
            mid_coef[n, block(i)] = parts[n]
    base = 192
    for c in range(2):
        for q in range(2):
            n = base + 32 * (2 * c + q)
            mid_state[c, q] = coarse[n : n + 32]
            a01_ref[c, q, 48:60, 0:256] = coarse[n + 4 : n + 16]
            a01_ref[c, q, 48:60, 256:512] = coarse[n + 16 : n + 28]
    for q in range(2):
        send_ref[4 + q] = mid_state[0, q, 8:24]
        packed_ref[4 + q] = mid_state[0, q, 8:24]

    def second_pair(n, carry):
        for source, target in ((s0, s1), (s1, s0)):
            run(source, target, 0, (1, 7))
            run(source, target, 1, (1, 7))
        return carry

    lax.fori_loop(0, 4, second_pair, 0)

    stacked = jnp.concatenate(
        [rows.coarsen(s0[c, q, 16:48]) for c in range(2) for q in range(2)], axis=0
    )
    coarse = exact_dot(stacked, down)
    for c in range(2):

        def load(i):
            return [mid_state[c, q, block(i)] for q in range(2)]

        def store(i, values):
            if 1 <= i < 3:
                for q in range(2):
                    n = 16 * (2 * c + q) + 8 * (i - 1)
                    forcing = coarse[n : n + 8] - values[q]
                    send_ref[2 * c + q, block(i - 1)] = forcing
                    packed_ref[2 * c + q, block(i - 1)] = forcing

        advance(load, store, lambda i: [mid_coef[n, block(i)] for n in range(6)], (0, 4))


def wide_mid_coefs(raw, coef_ref, lo_ref, hi_ref, mid_coef):
    for f in range(5):
        raw[f, 0:16] = lo_ref[6 + f]
        raw[f, 16:32] = coef_ref[6 + f]
        raw[f, 32:48] = hi_ref[6 + f]
    at = [raw[f, 4:44] for f in range(5)]
    parts = derived(2.0 * at[0], 2.0 * at[1], 8.0 * at[2], 8.0 * at[3], 8.0 * at[4])
    for n in range(6):
        mid_coef[n] = parts[n]


def mid_kernel(
    gathered_ref, own_ref, lo_ref, hi_ref, out_ref, coef_out_ref, raw, state, cells,
):
    rows = Rows(cells)
    wide_mid_coefs(raw, own_ref, lo_ref, hi_ref, coef_out_ref)

    def coeffs(i):
        return [coef_out_ref[n, block(i)] for n in range(6)]

    values = [[gathered_ref[0, 4 + q, block(i)] for q in range(2)] for i in range(5)]
    for step in range(8):
        holder, place = step // 2, step % 2

        def force(i):
            return [gathered_ref[holder, 2 * place + q, block(i)] for q in range(2)]

        values = advanced(values, coeffs, force)
    for i in range(5):
        for q in range(2):
            state[q, block(i)] = values[i][q]
    stacked = jnp.concatenate(
        [rows.coarsen(state[q, 12:28]) for q in range(2)]
        + [rows.coarsen(gathered_ref[0, 4 + q, 12:28]) for q in range(2)],
        axis=0,
    )
    coarse = exact_dot(stacked, down_matrix(256))
    for f in range(4):
        out_ref[f] = coarse[8 * f : 8 * f + 8]


def final_kernel(
    gathered_ref, top_ref, pred_ref, mid_coef, own_ref, lo_ref, hi_ref,
    a01_ref, a2_ref, w2_ref, fine_ref,
    result_ref,
    raw, low_coef, yz, series, cells, fine, w01, out_ref, sems,
):
    rows = Rows(cells)
    k, m = lax.axis_index("k"), lax.axis_index("m")
    for f in range(5):
        raw[f, 0:16] = lo_ref[6 + f]
        raw[f, 16:32] = own_ref[6 + f]
        raw[f, 32:48] = hi_ref[6 + f]
    down = down_matrix(256)
    up_low = up_matrix(256)
    stacked = jnp.concatenate([rows.coarsen(raw[f]) for f in range(5)], axis=0)
    coarse = exact_dot(stacked, down)
    at = [coarse[24 * f : 24 * f + 24] for f in range(5)]
    parts = derived(4.0 * at[0], 4.0 * at[1], 64.0 * at[2], 64.0 * at[3], 64.0 * at[4])
    for n in range(6):
        low_coef[n] = parts[n]

    def low_step(values):
        return advanced(values, lambda i: [low_coef[n, block(i)] for n in range(6)])

    def kept(slot):
        return [[yz[slot, q, block(i)] for q in range(2)] for i in range(3)]

    values = [[top_ref[RECEIVER[2], i, q] for q in range(2)] for i in range(3)]
    for back in (1, 0):
        follows = jnp.where(k - 1 - back > 0, F32(1.0), F32(0.0))
        other = low_step([[top_ref[RECEIVER[back], i, 2 + q] for q in range(2)] for i in range(3)])
        values = low_step(values)
        values = [
            [top_ref[RECEIVER[back], i, q] + follows * (values[i][q] - other[i][q]) for q in range(2)]
            for i in range(3)
        ]
    for i in range(3):
        for q in range(2):
            yz[0, q, block(i)] = values[i][q]
    stacked = jnp.concatenate(
        [rows.coarsen(gathered_ref[0, 4 + q]) for q in range(2)]
        + [rows.coarsen(w2_ref[q]) for q in range(2)]
        + [jnp.zeros((8, 256), F32)],
        axis=0,
    )
    coarse = exact_dot(stacked, down)
    inner = jnp.where(k > 0, F32(1.0), F32(0.0))
    fixes = []
    for q in range(2):
        z = coarse[20 * q : 20 * q + 20]
        yz[1, q] = jnp.zeros((24, 128), F32)
        yz[1, q, 2:22] = z
        fixes.append(inner * (yz[0, q, 2:22] - z))
    values, other = low_step(values), low_step(kept(1))
    for q in range(2):
        end = pred_ref[q] + inner * (values[1][q] - other[1][q])
        fixes.append(end - coarse[40 + 8 * q : 48 + 8 * q])
    fixes.append(jnp.zeros((8, 128), F32))
    refined = exact_dot(jnp.concatenate(fixes, axis=0), up_low)
    for q in range(2):
        series[0, q] = gathered_ref[0, 4 + q] + rows.repeat(refined[20 * q : 20 * q + 20])
        end = rows.repeat(refined[40 + 8 * q : 48 + 8 * q])
        series[8, q, 12:28] = w2_ref[q] + end

    values = [[series[0, q, block(i)] for q in range(2)] for i in range(5)]
    for step in range(7):
        holder, place = step // 2, step % 2

        def force(i):
            return [gathered_ref[holder, 2 * place + q, block(i)] for q in range(2)]

        values = advanced(values, lambda i: [mid_coef[n, block(i)] for n in range(6)], force)
        for i in range(5):
            for q in range(2):
                series[step + 1, q, block(i)] = values[i][q]

    changes = []
    for c in range(2):
        for q in range(2):
            w01[c, q, 0:12] = a01_ref[c, q, 48:60, 0:256]
            w01[c, q, 12:24] = a01_ref[c, q, 48:60, 256:512]
            changes.append(series[2 * m + c, q, 8:32] - w01[c, q])
    for q in range(2):
        changes.append(series[2 * m + 2, q, 12:28] - w2_ref[q])
    refined = exact_dot(jnp.concatenate(changes, axis=0), up_matrix(512))
    for c in range(2):
        for q in range(2):
            n = 2 * c + q
            fine[0, c, q] = a01_ref[c, q, 0:48] + rows.repeat(refined[24 * n : 24 * n + 24])
    for q in range(2):
        out_ref[15, q] = a2_ref[q] + rows.repeat(refined[96 + 16 * q : 112 + 16 * q])
        out_ref[7, q] = fine[0, 1, q, 8:40]

    def leave(n):
        return pltpu.make_async_copy(out_ref.at[n], result_ref.at[n], sems.at[n])

    leave(15).start()
    leave(7).start()

    def fine_step(source, target, position):
        for c in range(2):

            def load(i):
                return [fine[source, c, q, block(i)] for q in range(2)]

            def store(i, values):
                for q in range(2):
                    fine[target, c, q, block(i)] = values[q]
                    if 1 <= i < 5:
                        out_ref[8 * c + position, q, block(i - 1)] = values[q]

            advance(load, store, lambda i: [fine_ref[n, block(i)] for n in range(6)], (0, 6))
            leave(8 * c + position).start()

    def pair(n, carry):
        fine_step(0, 1, 2 * n)
        fine_step(1, 0, 2 * n + 1)
        return carry

    lax.fori_loop(0, 3, pair, 0)
    fine_step(0, 1, 6)
    for n in range(16):
        leave(n).wait()


def struct(*shape):
    return pltpu.VMEM(shape, F32)


def scratch(*shape):
    return pltpu.VMEM(shape, F32)


def limit(mib):
    return pltpu.CompilerParams(vmem_limit_bytes=mib * 2**20)


def near(x):
    return pltpu.with_memory_space_constraint(x, pltpu.VMEM)


def far(x):
    return pltpu.with_memory_space_constraint(x, pltpu.HBM)


def device(t, s):
    return t * N_SPACE + s


def send(x, dt, ds):
    pairs = [
        (device(t, s), device((t + dt) % N_TM, s + ds))
        for t in range(N_TM)
        for s in range(N_SPACE)
        if 0 <= s + ds < N_SPACE
    ]
    return lax.ppermute(x, AXES, pairs)


SENDER = (3, 2, 1)
RECEIVER = (1, 0, 3)


def from_group_behind(x, ds):
    pairs = []
    for k in range(GROUP):
        for back in range(k):
            for s in range(N_SPACE):
                if 0 <= s + ds < N_SPACE:
                    source = device(4 * (k - 1 - back) + SENDER[back], s + ds)
                    pairs.append((source, device(4 * k + RECEIVER[back], s)))
    return lax.ppermute(x, AXES, pairs)


def local(initial, guess, kappa, feed, kill, react):
    own, low_edge, high_edge = pl.pallas_call(
        pack_kernel,
        out_shape=(struct(9, 32, 512), struct(9, 16, 512), struct(9, 16, 512)),
        in_specs=[HBM] * 6,
        out_specs=(VMEM,) * 3,
        scratch_shapes=[pltpu.SemaphoreType.DMA((18,))],
        compiler_params=limit(4),
    )(*[far(x) for x in (initial, guess, kappa, feed, kill, react)])
    lo = send(low_edge, 0, 1)
    hi = send(high_edge, 0, -1)
    a01, a2, w2, held, packed, fine = pl.pallas_call(
        fine_kernel,
        out_shape=(
            struct(2, 2, 60, 512), struct(2, 32, 512), struct(2, 16, 256),
            struct(6, 16, 256), struct(11, 16, 256), struct(6, 48, 512),
        ),
        in_specs=[VMEM] * 3,
        out_specs=(VMEM,) * 6,
        scratch_shapes=[
            scratch(2, 2, 64, 512), scratch(2, 2, 64, 512), scratch(5, 64, 512),
            scratch(6, 64, 512), scratch(2, 2, 32, 256), scratch(6, 32, 256),
            scratch(60, 64, 128),
        ],
        compiler_params=limit(14),
    )(near(own), near(lo), near(hi))
    lo = send(packed, 1, 1)
    hi = send(packed, 1, -1)
    middle = send(held, 1, 0)
    window = jnp.concatenate([lo[:6, 4:], middle, hi[:6, :12]], axis=1)
    gathered = lax.all_gather(window, "m", axis=0, tiled=False)
    gathered, a01 = lax.optimization_barrier((gathered, a01))
    a01 = send(a01, 1, 0)
    pred, mid_coef = pl.pallas_call(
        mid_kernel,
        out_shape=(struct(4, 8, 128), struct(6, 40, 256)),
        in_specs=[VMEM] * 4,
        out_specs=(VMEM,) * 2,
        scratch_shapes=[scratch(5, 48, 256), scratch(2, 40, 256), scratch(8, 16, 128)],
        compiler_params=limit(8),
    )(near(gathered), near(packed), near(lo), near(hi))
    pieces = [from_group_behind(pred, ds) for ds in (-1, 0, 1)]
    top = lax.all_gather(jnp.stack(pieces), "m", axis=0, tiled=False)
    return pl.pallas_call(
        final_kernel,
        out_shape=jax.ShapeDtypeStruct((16, 2, 32, 512), F32),
        in_specs=[VMEM] * 11,
        out_specs=HBM,
        scratch_shapes=[
            scratch(5, 48, 256), scratch(6, 24, 128), scratch(2, 2, 24, 128),
            scratch(9, 2, 40, 256), scratch(50, 48, 128), scratch(2, 2, 2, 48, 512),
            scratch(2, 2, 24, 256), scratch(16, 2, 32, 512), pltpu.SemaphoreType.DMA((16,)),
        ],
        compiler_params=limit(18),
    )(*[near(x) for x in (gathered, top, pred, mid_coef, packed, lo, hi, a01, a2, w2, fine)])


def solution(mesh):
    split = Mesh(mesh.devices.reshape(4, 4, 16), AXES)
    tm = ("k", "m")
    placed = (
        P(None, "space", None),
        P(tm, None, "space", None),
        P(None, "space", None),
        P("space", None),
        P("space", None),
        P("space", None),
    )
    return jax.shard_map(
        local, mesh=split, in_specs=placed, out_specs=P(tm, None, "space", None), check_vma=False
    )
```

```python
import jax
import jax.numpy as jnp
from jax import lax
from jax.experimental import pallas as pl
from jax.experimental.pallas import tpu as pltpu
from jax.sharding import Mesh
from jax.sharding import PartitionSpec as P

F32 = jnp.float32
AXES = ("k", "m", "space")
VMEM = pl.BlockSpec(memory_space=pltpu.VMEM)
HBM = pl.BlockSpec(memory_space=pltpu.HBM)
N_TM = 16
N_SPACE = 16
GROUP = 4
STRIP = 32


def exact_dot(x, matrix):
    high = x.astype(jnp.bfloat16)
    rest = x - high.astype(F32)
    middle = rest.astype(jnp.bfloat16)
    low = (rest - middle.astype(F32)).astype(jnp.bfloat16)

    def part(piece):
        return lax.dot_general(
            piece, matrix, (((1,), (0,)), ((), ())), preferred_element_type=F32
        )

    return part(low) + part(middle) + part(high)


def down_matrix(fine):
    rows = lax.broadcasted_iota(jnp.int32, (fine, fine // 2), 0)
    cols = lax.broadcasted_iota(jnp.int32, (fine, fine // 2), 1)
    inside = (rows == 2 * cols) | (rows == 2 * cols + 1)
    return jnp.where(inside, F32(0.25), F32(0.0)).astype(jnp.bfloat16)


def up_matrix(fine):
    rows = lax.broadcasted_iota(jnp.int32, (fine // 2, fine), 0)
    cols = lax.broadcasted_iota(jnp.int32, (fine // 2, fine), 1)
    inside = (cols == 2 * rows) | (cols == 2 * rows + 1)
    return jnp.where(inside, F32(1.0), F32(0.0)).astype(jnp.bfloat16)


def split_tiles(x):
    return [x[:, 128 * k : 128 * k + 128] for k in range(x.shape[1] // 128)]


def side_sums(tiles, lane_first, lane_last):
    right_going = [pltpu.roll(t, 1, 1) for t in tiles]
    left_going = [pltpu.roll(t, 127, 1) for t in tiles]
    zero = jnp.zeros_like(tiles[0])
    out = []
    for k in range(len(tiles)):
        before = right_going[k - 1] if k > 0 else zero
        after = left_going[k + 1] if k < len(tiles) - 1 else zero
        out.append(
            jnp.where(lane_first, before, right_going[k])
            + jnp.where(lane_last, after, left_going[k])
        )
    return out


def advance(load, store, coeffs, blocks, force=None):
    sub = lax.broadcasted_iota(jnp.int32, (8, 128), 0)
    lane = lax.broadcasted_iota(jnp.int32, (8, 128), 1)
    first_row, last_row = sub == 0, sub == 7
    first_lane, last_lane = lane == 0, lane == 127
    held = {}

    def fetch(i):
        if i not in held:
            species = []
            for x in load(i):
                tiles = split_tiles(x)
                species.append(
                    (
                        tiles,
                        [pltpu.roll(t, 1, 0) for t in tiles],
                        [pltpu.roll(t, 7, 0) for t in tiles],
                    )
                )
            held[i] = species
        return held[i]

    low, high = blocks
    for i in range(low, high):
        here = fetch(i)
        above = fetch(max(i - 1, low))
        below = fetch(min(i + 1, high - 1))
        held.pop(i - 2, None)
        c = coeffs(i)
        sums = []
        for q in range(2):
            tiles, down, up = here[q]
            sides = side_sums(tiles, first_lane, last_lane)
            sums.append(
                [
                    jnp.where(first_row, above[q][1][k], down[k])
                    + jnp.where(last_row, below[q][2][k], up[k])
                    + sides[k]
                    for k in range(len(tiles))
                ]
            )
        next_a, next_b = [], []
        spread_a, spread_b, supply, keep_a, keep_b, coupling = [split_tiles(x) for x in c]
        for k in range(len(sums[0])):
            a, b = here[0][0][k], here[1][0][k]
            coupled = coupling[k] * a * b * b
            next_a.append(keep_a[k] * a + spread_a[k] * sums[0][k] + (supply[k] - coupled))
            next_b.append(keep_b[k] * b + spread_b[k] * sums[1][k] + coupled)
        out = [jnp.concatenate(next_a, axis=1), jnp.concatenate(next_b, axis=1)]
        if force is not None:
            extra = force(i)
            out = [out[0] + extra[0], out[1] + extra[1]]
        store(i, out)


def advanced(values, coeffs, force=None):
    out = [None] * len(values)

    def store(i, new):
        out[i] = new

    advance(lambda i: values[i], store, coeffs, (0, len(values)), force)
    return out


def derived(spread_a, spread_b, supply, removal, coupling):
    return (
        spread_a,
        spread_b,
        supply,
        1.0 - supply - 4.0 * spread_a,
        1.0 - supply - removal - 4.0 * spread_b,
        coupling,
    )


def block(i):
    return slice(8 * i, 8 * i + 8)


class Rows:
    def __init__(self, ref):
        self.ref, self.used = ref, 0

    def coarsen(self, x):
        count = x.shape[0]
        parts = []
        for tile in split_tiles(x):
            n = self.used
            self.used += 1
            self.ref[n, 0:count] = tile
            even = self.ref[n, pl.ds(0, count // 2, stride=2)]
            parts.append(even + self.ref[n, pl.ds(1, count // 2, stride=2)])
        return jnp.concatenate(parts, axis=1)

    def repeat(self, x):
        count = x.shape[0]
        parts = []
        for tile in split_tiles(x):
            n = self.used
            self.used += 1
            self.ref[n, pl.ds(0, count, stride=2)] = tile
            self.ref[n, pl.ds(1, count, stride=2)] = tile
            parts.append(self.ref[n, 0 : 2 * count])
        return jnp.concatenate(parts, axis=1)


def pack_kernel(
    initial_ref, guess_ref, kappa_ref, feed_ref, kill_ref, react_ref,
    own_ref, first_ref, second_ref, sems,
):
    last = GROUP * lax.axis_index("k") + lax.axis_index("m") == N_TM - 1
    count = [0]

    def copy(source, target):
        n = count[0]
        count[0] += 1
        return pltpu.make_async_copy(source, target, sems.at[n])

    def copies(pick, place, many, top, bottom):
        out = []
        at = pl.ds(place, many) if many > 1 else place
        for target, low, size in ((own_ref, 0, 32), (first_ref, top, 16), (second_ref, bottom, 16)):
            out.append(copy(pick(pl.ds(low, size)), target.at[at]))
        return out

    def all_copies(top, bottom, pick_end):
        count[0] = 0
        out = copies(lambda r: guess_ref.at[7, :, r], 5, 2, top, bottom)
        out += copies(lambda r: kappa_ref.at[:, r], 0, 2, top, bottom)
        out += copies(lambda r: feed_ref.at[r], 2, 1, top, bottom)
        out += copies(lambda r: kill_ref.at[r], 3, 1, top, bottom)
        out += copies(lambda r: react_ref.at[r], 4, 1, top, bottom)
        return out + copies(pick_end, 7, 2, top, bottom)

    odd = is_odd()
    for parity, top, bottom in ((odd, 16, 0), (jnp.logical_not(odd), 0, 16)):
        for at_end, pick in (
            (last, lambda r: initial_ref.at[:, r]),
            (jnp.logical_not(last), lambda r: guess_ref.at[15, :, r]),
        ):

            @pl.when(jnp.logical_and(parity, at_end))
            def _():
                for c in all_copies(top, bottom, pick):
                    c.start()

    for c in all_copies(16, 0, lambda r: guess_ref.at[15, :, r]):
        c.wait()


def fine_kernel(
    own_ref, first_ref, second_ref,
    a01_ref, a2_ref, w2_ref, packed_ref, send_ref, fine_ref,
    s0, s1, raw, tall, mid_state, mid_coef, cells,
):
    rows = Rows(cells)
    odd = is_odd()

    def lo(f):
        return jnp.where(odd, second_ref[f], first_ref[f])

    def hi(f):
        return jnp.where(odd, first_ref[f], second_ref[f])

    last = GROUP * lax.axis_index("k") + lax.axis_index("m") == N_TM - 1
    for c in range(2):
        for q in range(2):
            f = 5 + 2 * c + q
            s0[c, q, 0:16] = lo(f)
            s0[c, q, 16:48] = own_ref[f]
            s0[c, q, 48:64] = hi(f)
    for f in range(5):
        raw[f, 0:16] = lo(f)
        raw[f, 16:48] = own_ref[f]
        raw[f, 48:64] = hi(f)
    for i in range(8):
        r = block(i)
        parts = derived(*[raw[f, r] for f in range(5)])
        for n in range(6):
            tall[n, r] = parts[n]
        if 1 <= i < 7:
            for n in range(6):
                fine_ref[n, block(i - 1)] = parts[n]

    def coeffs(i):
        return [tall[n, block(i)] for n in range(6)]

    def run(source, target, chain, blocks):
        def load(i):
            return [source[chain, q, block(i)] for q in range(2)]

        def store(i, values):
            for q in range(2):
                target[chain, q, block(i)] = values[q]

        advance(load, store, coeffs, blocks)

    def first_pair(n, carry):
        for source, target in ((s0, s1), (s1, s0)):
            run(source, target, 0, (0, 8))
            run(source, target, 1, (0, 8))
        return carry

    lax.fori_loop(0, 4, first_pair, 0)

    for q in range(2):
        a2_ref[q] = s0[0, q, 16:48]
    stacked = [rows.coarsen(s0[0, q, 16:48]) for q in range(2)]
    for q in range(2):
        s0[0, q, 0:16] = jnp.where(last, lo(7 + q), s0[0, q, 0:16])
        s0[0, q, 16:48] = jnp.where(last, own_ref[7 + q], s0[0, q, 16:48])
        s0[0, q, 48:64] = jnp.where(last, hi(7 + q), s0[0, q, 48:64])
    for q in range(2):
        for c in range(2):
            a01_ref[c, q, 0:48] = s0[c, q, 8:56]

    stacked += [rows.coarsen(raw[f]) for f in range(5)]
    stacked += [rows.coarsen(s0[c, q]) for c in range(2) for q in range(2)]
    down = down_matrix(512)
    coarse = exact_dot(jnp.concatenate(stacked, axis=0), down)
    for q in range(2):
        w2_ref[q] = coarse[16 * q : 16 * q + 16]
    base = 32
    for f in range(5):
        send_ref[6 + f] = coarse[base + 32 * f + 8 : base + 32 * f + 24]
    for i in range(4):
        at = [coarse[base + 32 * f + 8 * i : base + 32 * f + 8 * i + 8] for f in range(5)]
        parts = derived(2.0 * at[0], 2.0 * at[1], 8.0 * at[2], 8.0 * at[3], 8.0 * at[4])
        for n in range(6):
            mid_coef[n, block(i)] = parts[n]
    base = 192
    for c in range(2):
        for q in range(2):
            n = base + 32 * (2 * c + q)
            mid_state[c, q] = coarse[n : n + 32]
            a01_ref[c, q, 48:60, 0:256] = coarse[n + 4 : n + 16]
            a01_ref[c, q, 48:60, 256:512] = coarse[n + 16 : n + 28]
    for q in range(2):
        send_ref[4 + q] = mid_state[0, q, 8:24]
        packed_ref[4 + q] = mid_state[0, q, 8:24]

    def second_pair(n, carry):
        for source, target in ((s0, s1), (s1, s0)):
            run(source, target, 0, (1, 7))
            run(source, target, 1, (1, 7))
        return carry

    lax.fori_loop(0, 4, second_pair, 0)

    stacked = jnp.concatenate(
        [rows.coarsen(s0[c, q, 16:48]) for c in range(2) for q in range(2)], axis=0
    )
    coarse = exact_dot(stacked, down)
    for c in range(2):

        def load(i):
            return [mid_state[c, q, block(i)] for q in range(2)]

        def store(i, values):
            if 1 <= i < 3:
                for q in range(2):
                    n = 16 * (2 * c + q) + 8 * (i - 1)
                    forcing = coarse[n : n + 8] - values[q]
                    send_ref[2 * c + q, block(i - 1)] = forcing
                    packed_ref[2 * c + q, block(i - 1)] = forcing

        advance(load, store, lambda i: [mid_coef[n, block(i)] for n in range(6)], (0, 4))


def wide_raw(raw, coef_ref, first_ref, second_ref):
    odd = is_odd()
    for f in range(5):
        first, second = first_ref[6 + f], second_ref[6 + f]
        raw[f, 0:16] = jnp.where(odd, second, first)
        raw[f, 16:32] = coef_ref[6 + f]
        raw[f, 32:48] = jnp.where(odd, first, second)


def wide_mid_coefs(raw, coef_ref, first_ref, second_ref, mid_coef):
    wide_raw(raw, coef_ref, first_ref, second_ref)
    at = [raw[f, 4:44] for f in range(5)]
    parts = derived(2.0 * at[0], 2.0 * at[1], 8.0 * at[2], 8.0 * at[3], 8.0 * at[4])
    for n in range(6):
        mid_coef[n] = parts[n]


def mid_kernel(
    gathered_ref, own_ref, first_ref, second_ref, out_ref, coef_out_ref, raw, state, cells,
):
    rows = Rows(cells)
    wide_mid_coefs(raw, own_ref, first_ref, second_ref, coef_out_ref)

    def coeffs(i):
        return [coef_out_ref[n, block(i)] for n in range(6)]

    values = [[gathered_ref[0, 4 + q, block(i)] for q in range(2)] for i in range(5)]
    for step in range(8):
        holder, place = step // 2, step % 2

        def force(i):
            return [gathered_ref[holder, 2 * place + q, block(i)] for q in range(2)]

        values = advanced(values, coeffs, force)
    for i in range(5):
        for q in range(2):
            state[q, block(i)] = values[i][q]
    stacked = jnp.concatenate(
        [rows.coarsen(state[q, 12:28]) for q in range(2)]
        + [rows.coarsen(gathered_ref[0, 4 + q, 12:28]) for q in range(2)],
        axis=0,
    )
    coarse = exact_dot(stacked, down_matrix(256))
    for f in range(4):
        out_ref[f] = coarse[8 * f : 8 * f + 8]


def final_kernel(
    gathered_ref, top_ref, pred_ref, mid_coef, own_ref, first_ref, second_ref,
    a01_ref, a2_ref, w2_ref, fine_ref,
    result_ref,
    raw, low_coef, yz, series, cells, fine, w01, out_ref, sems,
):
    rows = Rows(cells)
    k, m = lax.axis_index("k"), lax.axis_index("m")
    wide_raw(raw, own_ref, first_ref, second_ref)
    down = down_matrix(256)
    up_low = up_matrix(256)
    stacked = jnp.concatenate([rows.coarsen(raw[f]) for f in range(5)], axis=0)
    coarse = exact_dot(stacked, down)
    at = [coarse[24 * f : 24 * f + 24] for f in range(5)]
    parts = derived(4.0 * at[0], 4.0 * at[1], 64.0 * at[2], 64.0 * at[3], 64.0 * at[4])
    for n in range(6):
        low_coef[n] = parts[n]

    def low_step(values):
        return advanced(values, lambda i: [low_coef[n, block(i)] for n in range(6)])

    def kept(slot):
        return [[yz[slot, q, block(i)] for q in range(2)] for i in range(3)]

    values = [[top_ref[RECEIVER[2], i, q] for q in range(2)] for i in range(3)]
    for back in (1, 0):
        follows = jnp.where(k - 1 - back > 0, F32(1.0), F32(0.0))
        other = low_step([[top_ref[RECEIVER[back], i, 2 + q] for q in range(2)] for i in range(3)])
        values = low_step(values)
        values = [
            [top_ref[RECEIVER[back], i, q] + follows * (values[i][q] - other[i][q]) for q in range(2)]
            for i in range(3)
        ]
    for i in range(3):
        for q in range(2):
            yz[0, q, block(i)] = values[i][q]
    stacked = jnp.concatenate(
        [rows.coarsen(gathered_ref[0, 4 + q]) for q in range(2)]
        + [rows.coarsen(w2_ref[q]) for q in range(2)]
        + [jnp.zeros((8, 256), F32)],
        axis=0,
    )
    coarse = exact_dot(stacked, down)
    inner = jnp.where(k > 0, F32(1.0), F32(0.0))
    fixes = []
    for q in range(2):
        z = coarse[20 * q : 20 * q + 20]
        yz[1, q] = jnp.zeros((24, 128), F32)
        yz[1, q, 2:22] = z
        fixes.append(inner * (yz[0, q, 2:22] - z))
    values, other = low_step(values), low_step(kept(1))
    for q in range(2):
        end = pred_ref[q] + inner * (values[1][q] - other[1][q])
        fixes.append(end - coarse[40 + 8 * q : 48 + 8 * q])
    fixes.append(jnp.zeros((8, 128), F32))
    refined = exact_dot(jnp.concatenate(fixes, axis=0), up_low)
    for q in range(2):
        series[0, q] = gathered_ref[0, 4 + q] + rows.repeat(refined[20 * q : 20 * q + 20])
        end = rows.repeat(refined[40 + 8 * q : 48 + 8 * q])
        series[8, q, 12:28] = w2_ref[q] + end

    values = [[series[0, q, block(i)] for q in range(2)] for i in range(5)]
    for step in range(7):
        holder, place = step // 2, step % 2

        def force(i):
            return [gathered_ref[holder, 2 * place + q, block(i)] for q in range(2)]

        values = advanced(values, lambda i: [mid_coef[n, block(i)] for n in range(6)], force)
        for i in range(5):
            for q in range(2):
                series[step + 1, q, block(i)] = values[i][q]

    changes = []
    for c in range(2):
        for q in range(2):
            w01[c, q, 0:12] = a01_ref[c, q, 48:60, 0:256]
            w01[c, q, 12:24] = a01_ref[c, q, 48:60, 256:512]
            changes.append(series[2 * m + c, q, 8:32] - w01[c, q])
    for q in range(2):
        changes.append(series[2 * m + 2, q, 12:28] - w2_ref[q])
    refined = exact_dot(jnp.concatenate(changes, axis=0), up_matrix(512))
    for c in range(2):
        for q in range(2):
            n = 2 * c + q
            fine[0, c, q] = a01_ref[c, q, 0:48] + rows.repeat(refined[24 * n : 24 * n + 24])
    for q in range(2):
        out_ref[15, q] = a2_ref[q] + rows.repeat(refined[96 + 16 * q : 112 + 16 * q])
        out_ref[7, q] = fine[0, 1, q, 8:40]

    def leave(n):
        return pltpu.make_async_copy(out_ref.at[n], result_ref.at[n], sems.at[n])

    leave(15).start()
    leave(7).start()

    def fine_step(source, target, position):
        for c in range(2):

            def load(i):
                return [fine[source, c, q, block(i)] for q in range(2)]

            def store(i, values):
                for q in range(2):
                    fine[target, c, q, block(i)] = values[q]
                    if 1 <= i < 5:
                        out_ref[8 * c + position, q, block(i - 1)] = values[q]

            advance(load, store, lambda i: [fine_ref[n, block(i)] for n in range(6)], (0, 6))
            leave(8 * c + position).start()

    def pair(n, carry):
        fine_step(0, 1, 2 * n)
        fine_step(1, 0, 2 * n + 1)
        return carry

    lax.fori_loop(0, 3, pair, 0)
    fine_step(0, 1, 6)
    for n in range(16):
        leave(n).wait()


def struct(*shape):
    return pltpu.VMEM(shape, F32)


def scratch(*shape):
    return pltpu.VMEM(shape, F32)


def limit(mib):
    return pltpu.CompilerParams(vmem_limit_bytes=mib * 2**20)


def near(x):
    return pltpu.with_memory_space_constraint(x, pltpu.VMEM)


def far(x):
    return pltpu.with_memory_space_constraint(x, pltpu.HBM)


def device(t, s):
    return t * N_SPACE + s


def shift(x):
    pairs = [
        (device(t, s), device((t + 1) % N_TM, s)) for t in range(N_TM) for s in range(N_SPACE)
    ]
    return lax.ppermute(x, AXES, pairs)


def swap(x, dt, first):
    pairs = []
    for t in range(N_TM):
        for s in range(N_SPACE):
            beside = s + 1 if (s % 2 == 1) == first else s - 1
            if 0 <= beside < N_SPACE:
                pairs.append((device(t, s), device((t + dt) % N_TM, beside)))
    return lax.ppermute(x, AXES, pairs)


def is_odd():
    return lax.axis_index("space") % 2 == 1


SENDER = (3, 2, 1)
RECEIVER = (1, 0, 3)


def from_group_behind(x, ds):
    pairs = []
    for k in range(GROUP):
        for back in range(k):
            for s in range(N_SPACE):
                if 0 <= s + ds < N_SPACE:
                    source = device(4 * (k - 1 - back) + SENDER[back], s + ds)
                    pairs.append((source, device(4 * k + RECEIVER[back], s)))
    return lax.ppermute(x, AXES, pairs)


def local(initial, guess, kappa, feed, kill, react):
    own, first_edge, second_edge = pl.pallas_call(
        pack_kernel,
        out_shape=(struct(9, 32, 512), struct(9, 16, 512), struct(9, 16, 512)),
        in_specs=[HBM] * 6,
        out_specs=(VMEM,) * 3,
        scratch_shapes=[pltpu.SemaphoreType.DMA((18,))],
        compiler_params=limit(4),
    )(*[far(x) for x in (initial, guess, kappa, feed, kill, react)])
    first = swap(first_edge, 0, True)
    second = swap(second_edge, 0, False)
    a01, a2, w2, held, packed, fine = pl.pallas_call(
        fine_kernel,
        out_shape=(
            struct(2, 2, 60, 512), struct(2, 32, 512), struct(2, 16, 256),
            struct(6, 16, 256), struct(11, 16, 256), struct(6, 48, 512),
        ),
        in_specs=[VMEM] * 3,
        out_specs=(VMEM,) * 6,
        scratch_shapes=[
            scratch(2, 2, 64, 512), scratch(2, 2, 64, 512), scratch(5, 64, 512),
            scratch(6, 64, 512), scratch(2, 2, 32, 256), scratch(6, 32, 256),
            scratch(60, 64, 128),
        ],
        compiler_params=limit(14),
    )(near(own), near(first), near(second))
    first = swap(packed, 1, True)
    second = swap(packed, 1, False)
    middle = shift(held)
    odd = is_odd()
    window = jnp.concatenate(
        [
            jnp.where(odd, second[:6, 4:], first[:6, 4:]),
            middle,
            jnp.where(odd, first[:6, :12], second[:6, :12]),
        ],
        axis=1,
    )
    gathered = lax.all_gather(window, "m", axis=0, tiled=False)
    gathered, a01 = lax.optimization_barrier((gathered, a01))
    a01 = shift(a01)
    pred, mid_coef = pl.pallas_call(
        mid_kernel,
        out_shape=(struct(4, 8, 128), struct(6, 40, 256)),
        in_specs=[VMEM] * 4,
        out_specs=(VMEM,) * 2,
        scratch_shapes=[scratch(5, 48, 256), scratch(2, 40, 256), scratch(8, 16, 128)],
        compiler_params=limit(8),
    )(near(gathered), near(packed), near(first), near(second))
    pieces = [from_group_behind(pred, ds) for ds in (-1, 0, 1)]
    top = lax.all_gather(jnp.stack(pieces), "m", axis=0, tiled=False)
    return pl.pallas_call(
        final_kernel,
        out_shape=jax.ShapeDtypeStruct((16, 2, 32, 512), F32),
        in_specs=[VMEM] * 11,
        out_specs=HBM,
        scratch_shapes=[
            scratch(5, 48, 256), scratch(6, 24, 128), scratch(2, 2, 24, 128),
            scratch(9, 2, 40, 256), scratch(50, 48, 128), scratch(2, 2, 2, 48, 512),
            scratch(2, 2, 24, 256), scratch(16, 2, 32, 512), pltpu.SemaphoreType.DMA((16,)),
        ],
        compiler_params=limit(18),
    )(*[near(x) for x in (gathered, top, pred, mid_coef, packed, first, second, a01, a2, w2, fine)])


def solution(mesh):
    split = Mesh(mesh.devices.reshape(4, 4, 16), AXES)
    tm = ("k", "m")
    placed = (
        P(None, "space", None),
        P(tm, None, "space", None),
        P(None, "space", None),
        P("space", None),
        P("space", None),
        P("space", None),
    )
    return jax.shard_map(
        local, mesh=split, in_specs=placed, out_specs=P(tm, None, "space", None), check_vma=False
    )
```

```python
import jax
import jax.numpy as jnp
from jax import lax
from jax.experimental import pallas as pl
from jax.experimental.pallas import tpu as pltpu
from jax.sharding import Mesh
from jax.sharding import PartitionSpec as P

F32 = jnp.float32
AXES = ("k", "m", "space")
VMEM = pl.BlockSpec(memory_space=pltpu.VMEM)
HBM = pl.BlockSpec(memory_space=pltpu.HBM)
N_TM = 16
N_SPACE = 16
GROUP = 4
STRIP = 32


def exact_dot(x, matrix):
    high = x.astype(jnp.bfloat16)
    rest = x - high.astype(F32)
    middle = rest.astype(jnp.bfloat16)
    low = (rest - middle.astype(F32)).astype(jnp.bfloat16)

    def part(piece):
        return lax.dot_general(
            piece, matrix, (((1,), (0,)), ((), ())), preferred_element_type=F32
        )

    return part(low) + part(middle) + part(high)


def down_matrix(fine):
    rows = lax.broadcasted_iota(jnp.int32, (fine, fine // 2), 0)
    cols = lax.broadcasted_iota(jnp.int32, (fine, fine // 2), 1)
    inside = (rows == 2 * cols) | (rows == 2 * cols + 1)
    return jnp.where(inside, F32(0.25), F32(0.0)).astype(jnp.bfloat16)


def up_matrix(fine):
    rows = lax.broadcasted_iota(jnp.int32, (fine // 2, fine), 0)
    cols = lax.broadcasted_iota(jnp.int32, (fine // 2, fine), 1)
    inside = (cols == 2 * rows) | (cols == 2 * rows + 1)
    return jnp.where(inside, F32(1.0), F32(0.0)).astype(jnp.bfloat16)


def split_tiles(x):
    return [x[:, 128 * k : 128 * k + 128] for k in range(x.shape[1] // 128)]


def side_sums(tiles, lane_first, lane_last):
    right_going = [pltpu.roll(t, 1, 1) for t in tiles]
    left_going = [pltpu.roll(t, 127, 1) for t in tiles]
    zero = jnp.zeros_like(tiles[0])
    out = []
    for k in range(len(tiles)):
        before = right_going[k - 1] if k > 0 else zero
        after = left_going[k + 1] if k < len(tiles) - 1 else zero
        out.append(
            jnp.where(lane_first, before, right_going[k])
            + jnp.where(lane_last, after, left_going[k])
        )
    return out


def advance(load, store, coeffs, blocks, force=None):
    sub = lax.broadcasted_iota(jnp.int32, (8, 128), 0)
    lane = lax.broadcasted_iota(jnp.int32, (8, 128), 1)
    first_row, last_row = sub == 0, sub == 7
    first_lane, last_lane = lane == 0, lane == 127
    held = {}

    def fetch(i):
        if i not in held:
            species = []
            for x in load(i):
                tiles = split_tiles(x)
                species.append(
                    (
                        tiles,
                        [pltpu.roll(t, 1, 0) for t in tiles],
                        [pltpu.roll(t, 7, 0) for t in tiles],
                    )
                )
            held[i] = species
        return held[i]

    low, high = blocks
    for i in range(low, high):
        here = fetch(i)
        above = fetch(max(i - 1, low))
        below = fetch(min(i + 1, high - 1))
        held.pop(i - 2, None)
        c = coeffs(i)
        sums = []
        for q in range(2):
            tiles, down, up = here[q]
            sides = side_sums(tiles, first_lane, last_lane)
            sums.append(
                [
                    jnp.where(first_row, above[q][1][k], down[k])
                    + jnp.where(last_row, below[q][2][k], up[k])
                    + sides[k]
                    for k in range(len(tiles))
                ]
            )
        next_a, next_b = [], []
        spread_a, spread_b, supply, keep_a, keep_b, coupling = [split_tiles(x) for x in c]
        for k in range(len(sums[0])):
            a, b = here[0][0][k], here[1][0][k]
            coupled = coupling[k] * a * b * b
            next_a.append(keep_a[k] * a + spread_a[k] * sums[0][k] + (supply[k] - coupled))
            next_b.append(keep_b[k] * b + spread_b[k] * sums[1][k] + coupled)
        out = [jnp.concatenate(next_a, axis=1), jnp.concatenate(next_b, axis=1)]
        if force is not None:
            extra = force(i)
            out = [out[0] + extra[0], out[1] + extra[1]]
        store(i, out)


def advanced(values, coeffs, force=None):
    out = [None] * len(values)

    def store(i, new):
        out[i] = new

    advance(lambda i: values[i], store, coeffs, (0, len(values)), force)
    return out


def derived(spread_a, spread_b, supply, removal, coupling):
    return (
        spread_a,
        spread_b,
        supply,
        1.0 - supply - 4.0 * spread_a,
        1.0 - supply - removal - 4.0 * spread_b,
        coupling,
    )


def block(i):
    return slice(8 * i, 8 * i + 8)


class Rows:
    def __init__(self, ref):
        self.ref, self.used = ref, 0

    def coarsen(self, x):
        count = x.shape[0]
        parts = []
        for tile in split_tiles(x):
            n = self.used
            self.used += 1
            self.ref[n, 0:count] = tile
            even = self.ref[n, pl.ds(0, count // 2, stride=2)]
            parts.append(even + self.ref[n, pl.ds(1, count // 2, stride=2)])
        return jnp.concatenate(parts, axis=1)

    def repeat(self, x):
        count = x.shape[0]
        parts = []
        for tile in split_tiles(x):
            n = self.used
            self.used += 1
            self.ref[n, pl.ds(0, count, stride=2)] = tile
            self.ref[n, pl.ds(1, count, stride=2)] = tile
            parts.append(self.ref[n, 0 : 2 * count])
        return jnp.concatenate(parts, axis=1)


def pack_kernel(
    initial_ref, guess_ref, kappa_ref, feed_ref, kill_ref, react_ref,
    own_ref, first_ref, second_ref, sems,
):
    last = GROUP * lax.axis_index("k") + lax.axis_index("m") == N_TM - 1
    count = [0]

    def copy(source, target):
        n = count[0]
        count[0] += 1
        return pltpu.make_async_copy(source, target, sems.at[n])

    def copies(pick, place, many, top, bottom):
        out = []
        at = pl.ds(place, many) if many > 1 else place
        for target, low, size in ((own_ref, 0, 32), (first_ref, top, 16), (second_ref, bottom, 16)):
            out.append(copy(pick(pl.ds(low, size)), target.at[at]))
        return out

    def all_copies(top, bottom, pick_end):
        count[0] = 0
        out = copies(lambda r: guess_ref.at[7, :, r], 5, 2, top, bottom)
        out += copies(lambda r: kappa_ref.at[:, r], 0, 2, top, bottom)
        out += copies(lambda r: feed_ref.at[r], 2, 1, top, bottom)
        out += copies(lambda r: kill_ref.at[r], 3, 1, top, bottom)
        out += copies(lambda r: react_ref.at[r], 4, 1, top, bottom)
        return out + copies(pick_end, 7, 2, top, bottom)

    odd = is_odd()
    for parity, top, bottom in ((odd, 16, 0), (jnp.logical_not(odd), 0, 16)):
        for at_end, pick in (
            (last, lambda r: initial_ref.at[:, r]),
            (jnp.logical_not(last), lambda r: guess_ref.at[15, :, r]),
        ):

            @pl.when(jnp.logical_and(parity, at_end))
            def _():
                for c in all_copies(top, bottom, pick):
                    c.start()

    for c in all_copies(16, 0, lambda r: guess_ref.at[15, :, r]):
        c.wait()


def fine_kernel(
    own_ref, first_ref, second_ref,
    a01_ref, a2_ref, w2_ref, packed_ref, coarse_ref, to_first_ref, to_second_ref, fine_ref,
    s0, s1, raw, tall, mid_state, mid_coef, cells,
):
    rows = Rows(cells)
    odd = is_odd()

    def lo(f):
        return jnp.where(odd, second_ref[f], first_ref[f])

    def hi(f):
        return jnp.where(odd, first_ref[f], second_ref[f])

    last = GROUP * lax.axis_index("k") + lax.axis_index("m") == N_TM - 1
    for c in range(2):
        for q in range(2):
            f = 5 + 2 * c + q
            s0[c, q, 0:16] = lo(f)
            s0[c, q, 16:48] = own_ref[f]
            s0[c, q, 48:64] = hi(f)
    for f in range(5):
        raw[f, 0:16] = lo(f)
        raw[f, 16:48] = own_ref[f]
        raw[f, 48:64] = hi(f)
    for i in range(8):
        r = block(i)
        parts = derived(*[raw[f, r] for f in range(5)])
        for n in range(6):
            tall[n, r] = parts[n]
        if 1 <= i < 7:
            for n in range(6):
                fine_ref[n, block(i - 1)] = parts[n]

    def coeffs(i):
        return [tall[n, block(i)] for n in range(6)]

    def run(source, target, chain, blocks):
        def load(i):
            return [source[chain, q, block(i)] for q in range(2)]

        def store(i, values):
            for q in range(2):
                target[chain, q, block(i)] = values[q]

        advance(load, store, coeffs, blocks)

    def first_pair(n, carry):
        for source, target in ((s0, s1), (s1, s0)):
            run(source, target, 0, (0, 8))
            run(source, target, 1, (0, 8))
        return carry

    lax.fori_loop(0, 4, first_pair, 0)

    for q in range(2):
        a2_ref[q] = s0[0, q, 16:48]
    stacked = [rows.coarsen(s0[0, q, 16:48]) for q in range(2)]
    for q in range(2):
        s0[0, q, 0:16] = jnp.where(last, lo(7 + q), s0[0, q, 0:16])
        s0[0, q, 16:48] = jnp.where(last, own_ref[7 + q], s0[0, q, 16:48])
        s0[0, q, 48:64] = jnp.where(last, hi(7 + q), s0[0, q, 48:64])
    for q in range(2):
        for c in range(2):
            a01_ref[c, q, 0:48] = s0[c, q, 8:56]

    stacked += [rows.coarsen(raw[f]) for f in range(5)]
    stacked += [rows.coarsen(s0[c, q]) for c in range(2) for q in range(2)]
    down = down_matrix(512)
    coarse = exact_dot(jnp.concatenate(stacked, axis=0), down)
    for q in range(2):
        w2_ref[q] = coarse[16 * q : 16 * q + 16]
    base = 32
    for f in range(5):
        n = base + 32 * f
        coarse_ref[f] = coarse[n : n + 32]
        low, high = coarse[n + 8 : n + 16], coarse[n + 16 : n + 24]
        slot, r = 6 + f // 2, block(f % 2)
        to_first_ref[slot, r] = jnp.where(odd, low, high)
        to_second_ref[slot, r] = jnp.where(odd, high, low)
    for ref in (to_first_ref, to_second_ref):
        ref[8, 8:16] = jnp.zeros((8, 256), F32)
    for i in range(4):
        at = [coarse[base + 32 * f + 8 * i : base + 32 * f + 8 * i + 8] for f in range(5)]
        parts = derived(2.0 * at[0], 2.0 * at[1], 8.0 * at[2], 8.0 * at[3], 8.0 * at[4])
        for n in range(6):
            mid_coef[n, block(i)] = parts[n]
    base = 192
    for c in range(2):
        for q in range(2):
            n = base + 32 * (2 * c + q)
            mid_state[c, q] = coarse[n : n + 32]
            a01_ref[c, q, 48:60, 0:256] = coarse[n + 4 : n + 16]
            a01_ref[c, q, 48:60, 256:512] = coarse[n + 16 : n + 28]
    for q in range(2):
        to_first_ref[4 + q] = mid_state[0, q, 8:24]
        to_second_ref[4 + q] = mid_state[0, q, 8:24]
        packed_ref[4 + q] = mid_state[0, q, 8:24]

    def second_pair(n, carry):
        for source, target in ((s0, s1), (s1, s0)):
            run(source, target, 0, (1, 7))
            run(source, target, 1, (1, 7))
        return carry

    lax.fori_loop(0, 4, second_pair, 0)

    stacked = jnp.concatenate(
        [rows.coarsen(s0[c, q, 16:48]) for c in range(2) for q in range(2)], axis=0
    )
    coarse = exact_dot(stacked, down)
    for c in range(2):

        def load(i):
            return [mid_state[c, q, block(i)] for q in range(2)]

        def store(i, values):
            if 1 <= i < 3:
                for q in range(2):
                    n = 16 * (2 * c + q) + 8 * (i - 1)
                    forcing = coarse[n : n + 8] - values[q]
                    to_first_ref[2 * c + q, block(i - 1)] = forcing
                    to_second_ref[2 * c + q, block(i - 1)] = forcing
                    packed_ref[2 * c + q, block(i - 1)] = forcing

        advance(load, store, lambda i: [mid_coef[n, block(i)] for n in range(6)], (0, 4))


def wide_raw(raw, coef_ref, first_ref, second_ref):
    odd = is_odd()
    for f in range(5):
        slot, r = 6 + f // 2, block(f % 2)
        first, second = first_ref[slot, r], second_ref[slot, r]
        raw[f, 0:8] = jnp.where(odd, second, first)
        raw[f, 8:40] = coef_ref[f]
        raw[f, 40:48] = jnp.where(odd, first, second)


def wide_mid_coefs(raw, coef_ref, first_ref, second_ref, mid_coef):
    wide_raw(raw, coef_ref, first_ref, second_ref)
    at = [raw[f, 4:44] for f in range(5)]
    parts = derived(2.0 * at[0], 2.0 * at[1], 8.0 * at[2], 8.0 * at[3], 8.0 * at[4])
    for n in range(6):
        mid_coef[n] = parts[n]


def mid_kernel(
    gathered_ref, own_ref, first_ref, second_ref, out_ref, coef_out_ref, raw, state, cells,
):
    rows = Rows(cells)
    wide_mid_coefs(raw, own_ref, first_ref, second_ref, coef_out_ref)

    def coeffs(i):
        return [coef_out_ref[n, block(i)] for n in range(6)]

    values = [[gathered_ref[0, 4 + q, block(i)] for q in range(2)] for i in range(5)]
    for step in range(8):
        holder, place = step // 2, step % 2

        def force(i):
            return [gathered_ref[holder, 2 * place + q, block(i)] for q in range(2)]

        values = advanced(values, coeffs, force)
    for i in range(5):
        for q in range(2):
            state[q, block(i)] = values[i][q]
    stacked = jnp.concatenate(
        [rows.coarsen(state[q, 12:28]) for q in range(2)]
        + [rows.coarsen(gathered_ref[0, 4 + q, 12:28]) for q in range(2)],
        axis=0,
    )
    coarse = exact_dot(stacked, down_matrix(256))
    for f in range(4):
        out_ref[f] = coarse[8 * f : 8 * f + 8]


def final_kernel(
    gathered_ref, top_ref, pred_ref, mid_coef, own_ref, first_ref, second_ref,
    a01_ref, a2_ref, w2_ref, fine_ref,
    result_ref,
    raw, low_coef, yz, series, cells, fine, w01, out_ref, sems,
):
    rows = Rows(cells)
    k, m = lax.axis_index("k"), lax.axis_index("m")
    wide_raw(raw, own_ref, first_ref, second_ref)
    down = down_matrix(256)
    up_low = up_matrix(256)
    stacked = jnp.concatenate([rows.coarsen(raw[f]) for f in range(5)], axis=0)
    coarse = exact_dot(stacked, down)
    at = [coarse[24 * f : 24 * f + 24] for f in range(5)]
    parts = derived(4.0 * at[0], 4.0 * at[1], 64.0 * at[2], 64.0 * at[3], 64.0 * at[4])
    for n in range(6):
        low_coef[n] = parts[n]

    def low_step(values):
        return advanced(values, lambda i: [low_coef[n, block(i)] for n in range(6)])

    def kept(slot):
        return [[yz[slot, q, block(i)] for q in range(2)] for i in range(3)]

    values = [[top_ref[RECEIVER[2], i, q] for q in range(2)] for i in range(3)]
    for back in (1, 0):
        follows = jnp.where(k - 1 - back > 0, F32(1.0), F32(0.0))
        other = low_step([[top_ref[RECEIVER[back], i, 2 + q] for q in range(2)] for i in range(3)])
        values = low_step(values)
        values = [
            [top_ref[RECEIVER[back], i, q] + follows * (values[i][q] - other[i][q]) for q in range(2)]
            for i in range(3)
        ]
    for i in range(3):
        for q in range(2):
            yz[0, q, block(i)] = values[i][q]
    stacked = jnp.concatenate(
        [rows.coarsen(gathered_ref[0, 4 + q]) for q in range(2)]
        + [rows.coarsen(w2_ref[q]) for q in range(2)]
        + [jnp.zeros((8, 256), F32)],
        axis=0,
    )
    coarse = exact_dot(stacked, down)
    inner = jnp.where(k > 0, F32(1.0), F32(0.0))
    fixes = []
    for q in range(2):
        z = coarse[20 * q : 20 * q + 20]
        yz[1, q] = jnp.zeros((24, 128), F32)
        yz[1, q, 2:22] = z
        fixes.append(inner * (yz[0, q, 2:22] - z))
    values, other = low_step(values), low_step(kept(1))
    for q in range(2):
        end = pred_ref[q] + inner * (values[1][q] - other[1][q])
        fixes.append(end - coarse[40 + 8 * q : 48 + 8 * q])
    fixes.append(jnp.zeros((8, 128), F32))
    refined = exact_dot(jnp.concatenate(fixes, axis=0), up_low)
    for q in range(2):
        series[0, q] = gathered_ref[0, 4 + q] + rows.repeat(refined[20 * q : 20 * q + 20])
        end = rows.repeat(refined[40 + 8 * q : 48 + 8 * q])
        series[8, q, 12:28] = w2_ref[q] + end

    values = [[series[0, q, block(i)] for q in range(2)] for i in range(5)]
    for step in range(7):
        holder, place = step // 2, step % 2

        def force(i):
            return [gathered_ref[holder, 2 * place + q, block(i)] for q in range(2)]

        values = advanced(values, lambda i: [mid_coef[n, block(i)] for n in range(6)], force)
        for i in range(5):
            for q in range(2):
                series[step + 1, q, block(i)] = values[i][q]

    changes = []
    for c in range(2):
        for q in range(2):
            w01[c, q, 0:12] = a01_ref[c, q, 48:60, 0:256]
            w01[c, q, 12:24] = a01_ref[c, q, 48:60, 256:512]
            changes.append(series[2 * m + c, q, 8:32] - w01[c, q])
    for q in range(2):
        changes.append(series[2 * m + 2, q, 12:28] - w2_ref[q])
    refined = exact_dot(jnp.concatenate(changes, axis=0), up_matrix(512))
    for c in range(2):
        for q in range(2):
            n = 2 * c + q
            fine[0, c, q] = a01_ref[c, q, 0:48] + rows.repeat(refined[24 * n : 24 * n + 24])
    for q in range(2):
        out_ref[15, q] = a2_ref[q] + rows.repeat(refined[96 + 16 * q : 112 + 16 * q])
        out_ref[7, q] = fine[0, 1, q, 8:40]

    def leave(n):
        return pltpu.make_async_copy(out_ref.at[n], result_ref.at[n], sems.at[n])

    leave(15).start()
    leave(7).start()

    def fine_step(source, target, position):
        for c in range(2):

            def load(i):
                return [fine[source, c, q, block(i)] for q in range(2)]

            def store(i, values):
                for q in range(2):
                    fine[target, c, q, block(i)] = values[q]
                    if 1 <= i < 5:
                        out_ref[8 * c + position, q, block(i - 1)] = values[q]

            advance(load, store, lambda i: [fine_ref[n, block(i)] for n in range(6)], (0, 6))
            leave(8 * c + position).start()

    def pair(n, carry):
        fine_step(0, 1, 2 * n)
        fine_step(1, 0, 2 * n + 1)
        return carry

    lax.fori_loop(0, 3, pair, 0)
    fine_step(0, 1, 6)
    for n in range(16):
        leave(n).wait()


def struct(*shape):
    return pltpu.VMEM(shape, F32)


def scratch(*shape):
    return pltpu.VMEM(shape, F32)


def limit(mib):
    return pltpu.CompilerParams(vmem_limit_bytes=mib * 2**20)


def near(x):
    return pltpu.with_memory_space_constraint(x, pltpu.VMEM)


def far(x):
    return pltpu.with_memory_space_constraint(x, pltpu.HBM)


def device(t, s):
    return t * N_SPACE + s


def shift(x):
    pairs = [
        (device(t, s), device((t + 1) % N_TM, s)) for t in range(N_TM) for s in range(N_SPACE)
    ]
    return lax.ppermute(x, AXES, pairs)


def swap(x, dt, first):
    pairs = []
    for t in range(N_TM):
        for s in range(N_SPACE):
            beside = s + 1 if (s % 2 == 1) == first else s - 1
            if 0 <= beside < N_SPACE:
                pairs.append((device(t, s), device((t + dt) % N_TM, beside)))
    return lax.ppermute(x, AXES, pairs)


def is_odd():
    return lax.axis_index("space") % 2 == 1


SENDER = (3, 2, 1)
RECEIVER = (1, 0, 3)


def from_group_behind(x, ds):
    pairs = []
    for k in range(GROUP):
        for back in range(k):
            for s in range(N_SPACE):
                if 0 <= s + ds < N_SPACE:
                    source = device(4 * (k - 1 - back) + SENDER[back], s + ds)
                    pairs.append((source, device(4 * k + RECEIVER[back], s)))
    return lax.ppermute(x, AXES, pairs)


def local(initial, guess, kappa, feed, kill, react):
    own, first_edge, second_edge = pl.pallas_call(
        pack_kernel,
        out_shape=(struct(9, 32, 512), struct(9, 16, 512), struct(9, 16, 512)),
        in_specs=[HBM] * 6,
        out_specs=(VMEM,) * 3,
        scratch_shapes=[pltpu.SemaphoreType.DMA((18,))],
        compiler_params=limit(4),
    )(*[far(x) for x in (initial, guess, kappa, feed, kill, react)])
    first = swap(first_edge, 0, True)
    second = swap(second_edge, 0, False)
    a01, a2, w2, held, coarse, to_first, to_second, fine = pl.pallas_call(
        fine_kernel,
        out_shape=(
            struct(2, 2, 60, 512), struct(2, 32, 512), struct(2, 16, 256),
            struct(6, 16, 256), struct(5, 32, 256), struct(9, 16, 256), struct(9, 16, 256),
            struct(6, 48, 512),
        ),
        in_specs=[VMEM] * 3,
        out_specs=(VMEM,) * 8,
        scratch_shapes=[
            scratch(2, 2, 64, 512), scratch(2, 2, 64, 512), scratch(5, 64, 512),
            scratch(6, 64, 512), scratch(2, 2, 32, 256), scratch(6, 32, 256),
            scratch(60, 64, 128),
        ],
        compiler_params=limit(14),
    )(near(own), near(first), near(second))
    first = swap(to_first, 1, True)
    second = swap(to_second, 1, False)
    middle = shift(held)
    odd = is_odd()
    window = jnp.concatenate(
        [
            jnp.where(odd, second[:6, 4:], first[:6, 4:]),
            middle,
            jnp.where(odd, first[:6, :12], second[:6, :12]),
        ],
        axis=1,
    )
    gathered = lax.all_gather(window, "m", axis=0, tiled=False)
    gathered, a01 = lax.optimization_barrier((gathered, a01))
    a01 = shift(a01)
    pred, mid_coef = pl.pallas_call(
        mid_kernel,
        out_shape=(struct(4, 8, 128), struct(6, 40, 256)),
        in_specs=[VMEM] * 4,
        out_specs=(VMEM,) * 2,
        scratch_shapes=[scratch(5, 48, 256), scratch(2, 40, 256), scratch(8, 16, 128)],
        compiler_params=limit(8),
    )(near(gathered), near(coarse), near(first), near(second))
    pieces = [from_group_behind(pred, ds) for ds in (-1, 0, 1)]
    top = lax.all_gather(jnp.stack(pieces), "m", axis=0, tiled=False)
    return pl.pallas_call(
        final_kernel,
        out_shape=jax.ShapeDtypeStruct((16, 2, 32, 512), F32),
        in_specs=[VMEM] * 11,
        out_specs=HBM,
        scratch_shapes=[
            scratch(5, 48, 256), scratch(6, 24, 128), scratch(2, 2, 24, 128),
            scratch(9, 2, 40, 256), scratch(50, 48, 128), scratch(2, 2, 2, 48, 512),
            scratch(2, 2, 24, 256), scratch(16, 2, 32, 512), pltpu.SemaphoreType.DMA((16,)),
        ],
        compiler_params=limit(18),
    )(*[near(x) for x in (gathered, top, pred, mid_coef, coarse, first, second, a01, a2, w2, fine)])


def solution(mesh):
    split = Mesh(mesh.devices.reshape(4, 4, 16), AXES)
    tm = ("k", "m")
    placed = (
        P(None, "space", None),
        P(tm, None, "space", None),
        P(None, "space", None),
        P("space", None),
        P("space", None),
        P("space", None),
    )
    return jax.shard_map(
        local, mesh=split, in_specs=placed, out_specs=P(tm, None, "space", None), check_vma=False
    )
```
